256 devices in a mesh: span: 8 (over y, core), chord: 32 (over z, x).
Axes of the slice: x: 4, y: 4, z: 8, core: 2. Of those that a mesh axis runs over, the one named last changes fastest.
Arguments:
- node_pos: float32 [3, 524288], P(None, ('span', 'chord')), may hold values from -0.4 to 0.4
- ctrl_pos: float32 [3, 8192], P(None, ('span', 'chord')), may hold values from -0.4 to 0.4
- ctrl_ids: int32 [8192], P(('span', 'chord')), may hold values from 0 to 1023
- wing_shift: float32 [15, 1024], replicated, may hold values from -0.06 to 0.06
- wing_speed: float32 [15, 1024], replicated, may hold values from -0.6 to 0.6
- minv: float32 [8192, 8192], P(('span', 'chord')), may hold values from -1 to 3, as said below
- conn: int32 [64, 32768], P(None, ('span', 'chord')), may hold values from 0 to 2047
- face_elem: int32 [8, 32, 4, 32], P('span', 'chord'), may hold values from 0 to 127
- face_match: int32 [8, 32, 4, 32], P('span', 'chord'), may hold values from 0 to 31, each once within a row
Outputs:
- det_jac: float32 [5, 64, 32768], P(None, None, ('span', 'chord'))
- grid_flux: float32 [5, 3, 64, 32768], P(None, None, None, ('span', 'chord'))
- face_flux: float32 [8, 32, 4, 5, 16, 32], P('span', 'chord')
The draws below stay inside these ranges and needn't reach their ends.
Inputs may be any that keep to these rules, and one draw needn't show every extreme that they name: minv is exactly symmetric. Each face_match[j, k, t, :] is a permutation of 0 to 31.
All inputs are finite; a program needn't handle non-finite values.
Results may differ from the reference program's by a relative error of at most 0.00025.
Values sent between devices are 32-bit elements; how exact they have to be, the bound alone decides.
A program may use at most 64 MiB of HBM per device.

```python
import math
import jax
import jax.numpy as jnp
import numpy as np
from jax import lax

NC = 8192
NS = 1024
SECTIONS = 5
PTS = 64
E_DEV = 128
NODE_DEV = 2048
FB = 32
NODES = 524288
ELEMS = 32768
N_SPAN = 8
N_CHORD = 32


def draw_minv(key, part):
    noise_key, scale_key = jax.random.split(key)
    perturb = jax.random.truncated_normal(noise_key, -4.0, 4.0, (NC, NC), jnp.float32) * (0.5 / math.sqrt(NC))
    diagonal = jnp.exp(jax.random.uniform(scale_key, (NC,), jnp.float32, math.log(0.5), math.log(2.0)))
    return (perturb + perturb.T) * 0.7071 + jnp.diag(diagonal)


def with_ends(entries, key, least, high):
    extent = entries.shape
    index_at = [jax.random.randint(jax.random.fold_in(key, axis), (), 0, extent[axis]) for axis in range(len(extent))]
    entries = entries.at[tuple(index_at)].set(least)
    longest = extent.index(max(extent))
    index_at[longest] = (index_at[longest] + 1) % extent[longest]
    return entries.at[tuple(index_at)].set(high)


def block_scale(key, extent, shards, low, high):
    def one(dim, shards_of):
        steps = jax.random.uniform(jax.random.fold_in(jax.random.fold_in(key, 6), dim), (shards_of,), jnp.float32, low / len(shards), high / len(shards))
        return jnp.repeat(jnp.exp(steps), extent[dim] // shards_of).reshape((-1,) + (1,) * (len(extent) - dim - 1))

    factor_of = one(*shards[0])
    for cut in shards[1:]:
        factor_of = factor_of * one(*cut)
    return factor_of


def bell_draw(own_key, shape, width, reach, held_as=jnp.bfloat16):
    drawn = jax.random.normal(own_key, shape, jnp.float32) * width
    return jnp.minimum(jnp.maximum(drawn, -reach), reach).astype(held_as)


def setup_inputs(seed: int = 0) -> dict:
    splits = jax.random.split(jax.random.key(seed), 10)
    node_pos = jnp.clip(jax.random.uniform(splits[0], (3, NODES), jnp.float32, -0.4, 0.4) * block_scale(splits[0], (3, NODES), ((1, 256),), -0.4, 0.0), -0.4, 0.4)
    ctrl_pos = jnp.clip(jax.random.uniform(splits[1], (3, NC), jnp.float32, -0.4, 0.4) * block_scale(splits[1], (3, NC), ((1, 256),), -0.4, 0.0), -0.4, 0.4)
    ctrl_ids = with_ends(jax.random.randint(splits[2], (NC,), 0, NS), jax.random.fold_in(splits[2], 1), 0, NS - 1).astype(jnp.int32)
    wing_shift = bell_draw(splits[3], (3 * SECTIONS, NS), 0.01, 0.06, jnp.float32)
    wing_speed = bell_draw(splits[4], (3 * SECTIONS, NS), 0.1, 0.6, jnp.float32)
    minv = draw_minv(jax.random.fold_in(splits[9], 71), 0)
    conn = with_ends(jax.random.randint(splits[6], (PTS, ELEMS), 0, NODE_DEV), jax.random.fold_in(splits[6], 1), 0, NODE_DEV - 1).astype(jnp.int32)
    face_elem = with_ends(jax.random.randint(splits[7], (N_SPAN, N_CHORD, 4, FB), 0, E_DEV), jax.random.fold_in(splits[7], 1), 0, E_DEV - 1).astype(jnp.int32)
    face_match = jax.vmap(lambda own: jax.random.permutation(own, FB))(jax.random.split(splits[8], N_SPAN * N_CHORD * 4)).reshape((N_SPAN, N_CHORD, 4, FB)).astype(jnp.int32)
    return dict(node_pos=node_pos, ctrl_pos=ctrl_pos, ctrl_ids=ctrl_ids, wing_shift=wing_shift, wing_speed=wing_speed, minv=minv, conn=conn, face_elem=face_elem, face_match=face_match)


kernel_width = 0.1

def lobatto_table():
    points = np.array([-1.0, -1.0 / np.sqrt(5.0), 1.0 / np.sqrt(5.0), 1.0])
    barycentric = np.array([1.0 / np.prod([points[target] - points[source] for source in range(4) if source != target]) for target in range(4)])
    derivative = np.zeros((4, 4))
    for target in range(4):
        for source in range(4):
            if source != target:
                derivative[target, source] = barycentric[source] / barycentric[target] / (points[target] - points[source])
        derivative[target, target] = -np.sum(derivative[target])
    identity = np.eye(4)
    stacked = np.stack([np.kron(np.kron(derivative, identity), identity), np.kron(np.kron(identity, derivative), identity), np.kron(np.kron(identity, identity), derivative)])
    return stacked.reshape(192, 64)

def element_metrics(node_rows, positions, links):
    sections = node_rows.shape[0] // 6
    elements = links.shape[1]
    moved = node_rows[:3 * sections] + jnp.tile(positions, (sections, 1))
    gathered = jnp.take(jnp.concatenate([moved, node_rows[3 * sections:]], axis=0), links, axis=1)
    table = jnp.asarray(lobatto_table(), jnp.float32)
    jacobian = jnp.einsum('rq,kqe->rke', table, gathered[:3 * sections], precision=lax.Precision.HIGHEST)
    jacobian = jacobian.reshape(3, 64, sections, 3, elements).transpose(2, 3, 0, 1, 4)
    velocity = gathered[3 * sections:].reshape(sections, 3, 64, elements)

    def entry(spatial, along):
        return jacobian[:, spatial % 3, along % 3]
    metric = [[entry(spatial + 1, along + 1) * entry(spatial + 2, along + 2) - entry(spatial + 1, along + 2) * entry(spatial + 2, along + 1) for spatial in range(3)] for along in range(3)]
    volume = entry(0, 0) * metric[0][0] + entry(0, 1) * metric[1][0] + entry(0, 2) * metric[2][0]
    flux = jnp.stack([metric[along][0] * velocity[:, 0] + metric[along][1] * velocity[:, 1] + metric[along][2] * velocity[:, 2] for along in range(3)], axis=1)
    return (volume, flux)

def face_traces(flux, sides):
    sections, elements = (flux.shape[0], flux.shape[3])
    cube = flux.reshape(sections, 3, 4, 4, 4, elements)
    surfaces = [-cube[:, 2, :, :, 0], cube[:, 2, :, :, 3], -cube[:, 1, :, 0], cube[:, 1, :, 3]]
    return jnp.stack([jnp.take(surface.reshape(sections, 16, elements), sides[ordinal], axis=2) for ordinal, surface in enumerate(surfaces)])

def partition(arrays):
    node_rows, positions, links, sides = arrays
    volume, flux = element_metrics(node_rows, positions, links)
    return (volume, flux, face_traces(flux, sides))

def reference(node_pos, ctrl_pos, ctrl_ids, wing_shift, wing_speed, minv, conn, face_elem, face_match):
    highest = lax.Precision.HIGHEST
    devices = N_SPAN * N_CHORD
    table = jnp.concatenate([wing_shift, wing_speed], axis=0)
    right_side = jnp.take(table, ctrl_ids, axis=1)
    weights = jnp.dot(right_side, minv.T, precision=highest, preferred_element_type=jnp.float32)
    total_nodes = node_pos.shape[1]
    block_width = math.gcd(total_nodes, 4096)

    def motion_block(points):
        distance = (ctrl_pos[0][:, None] - points[0][None, :]) ** 2 + (ctrl_pos[1][:, None] - points[1][None, :]) ** 2 + (ctrl_pos[2][:, None] - points[2][None, :]) ** 2
        kernel = jnp.exp(-distance / (2.0 * kernel_width ** 2))
        return jnp.dot(weights, kernel, precision=highest, preferred_element_type=jnp.float32)
    blocks = node_pos.reshape(3, total_nodes // block_width, block_width).transpose(1, 0, 2)
    rows_count = table.shape[0]
    motion = lax.map(motion_block, blocks).transpose(1, 0, 2).reshape(rows_count, total_nodes)
    sections = rows_count // 6
    volume, flux, traces = lax.map(partition, (motion.reshape(rows_count, devices, NODE_DEV).transpose(1, 0, 2), node_pos.reshape(3, devices, NODE_DEV).transpose(1, 0, 2), conn.reshape(PTS, devices, E_DEV).transpose(1, 0, 2), face_elem.reshape(devices, 4, -1)))
    det_jac = volume.transpose(1, 2, 0, 3).reshape(sections, PTS, devices * E_DEV)
    grid_flux = flux.transpose(1, 2, 3, 0, 4).reshape(sections, 3, PTS, devices * E_DEV)
    traces = traces.reshape(N_SPAN, N_CHORD, 4, sections, 16, -1)
    received = jnp.stack([jnp.roll(traces[:, :, 1], 1, axis=0), jnp.roll(traces[:, :, 0], -1, axis=0), jnp.roll(traces[:, :, 3], 1, axis=1), jnp.roll(traces[:, :, 2], -1, axis=1)], axis=2)
    matched = jnp.take_along_axis(received, jnp.broadcast_to(face_match[:, :, :, None, None, :], received.shape), axis=5)
    span_index = jnp.arange(N_SPAN, dtype=jnp.int32)[:, None]
    side_index = jnp.arange(4, dtype=jnp.int32)[None, :]
    boundary = (span_index == 0) & (side_index == 0) | (span_index == N_SPAN - 1) & (side_index == 1)
    opposite = jnp.where(boundary[:, None, :, None, None, None], -traces, matched)
    face_flux = 0.5 * (traces - opposite)
    return (det_jac, grid_flux, face_flux)
```

```python
import functools

import jax
import jax.numpy as jnp
import numpy as np
from jax import lax
from jax.experimental import pallas as pl
from jax.experimental.pallas import tpu as pltpu
from jax.sharding import Mesh
from jax.sharding import PartitionSpec as P

SPAN_CHORD = ("y", "core", "z", "x")
SPAN = ("y", "core")
CHORD = ("z", "x")
NY, NCORE, NZ, NX = 4, 2, 8, 4
DEVICES = NY * NCORE * NZ * NX
GROUP = NCORE * NZ
MESH = pl.DeviceIdType.MESH
F32 = jnp.float32
BF16 = jnp.bfloat16

WIDTH = 0.1
HALF_INV = 1.0 / (2.0 * WIDTH**2)
CROSS = float(2.0 * HALF_INV * np.log2(np.e))
STORED = 22
TILES = 8


def lobatto_derivative():
    points = np.array([-1.0, -1.0 / np.sqrt(5.0), 1.0 / np.sqrt(5.0), 1.0])
    barycentric = np.array(
        [
            1.0 / np.prod([points[t] - points[s] for s in range(4) if s != t])
            for t in range(4)
        ]
    )
    derivative = np.zeros((4, 4))
    for t in range(4):
        for s in range(4):
            if s != t:
                derivative[t, s] = barycentric[s] / barycentric[t] / (points[t] - points[s])
        derivative[t, t] = -np.sum(derivative[t])
    return derivative


def split3(value):
    high = value.astype(BF16)
    rest = value - high.astype(F32)
    middle = rest.astype(BF16)
    low = (rest - middle.astype(F32)).astype(BF16)
    return high, middle, low


def one_hot(index, blocks):
    width = index.shape[1]
    block = jnp.floor(index * (1.0 / 128.0))
    lane = (index - block * 128.0).astype(BF16)
    block = jnp.broadcast_to(block.astype(BF16), (128, width))
    row = lax.broadcasted_iota(jnp.int32, (128, width), 0).astype(F32).astype(BF16)
    one = jnp.ones((128, width), BF16)
    zero = jnp.zeros((128, width), BF16)
    inner = jnp.where(row == jnp.broadcast_to(lane, (128, width)), one, zero)
    return jnp.concatenate(
        [jnp.where(block == jnp.full((128, width), b, BF16), inner, zero) for b in range(blocks)],
        axis=0,
    )


def kernel(
    ids_ref,
    ctrl_ref,
    nodes_ref,
    shift_ref,
    speed_ref,
    minv_ref,
    conn_ref,
    elem_ref,
    match_ref,
    det_ref,
    flux_ref,
    face_ref,
    own_ref,
    g1_ref,
    g2_ref,
    gp_ref,
    idr_ref,
    table_ref,
    r3_ref,
    m3_ref,
    cross_ref,
    wt_ref,
    scale_ref,
    wc_ref,
    kh_ref,
    kl_ref,
    cb0_ref,
    cb1_ref,
    ns_ref,
    t3_ref,
    gat_ref,
    fl_ref,
    tr_ref,
    rc_ref,
    send1,
    recv1,
    send2,
    recv2,
    send3,
    recv3,
    send4,
    recv4,
    send5,
    recv5,
    send6,
    recv6,
):
    y, core, z, x = (lax.axis_index(name) for name in SPAN_CHORD)
    group = y * NX + x
    place = core * NZ + z
    line = [(dc, dz) for dc in range(NCORE) for dz in range(NZ) if (dc, dz) != (0, 0)]
    plane = [(dy, dx) for dy in range(NY) for dx in range(NX) if (dy, dx) != (0, 0)]

    def line_device(dc, dz):
        return (y, lax.rem(core + dc, NCORE), lax.rem(z + dz, NZ), x)

    def plane_device(dy, dx):
        return (lax.rem(y + dy, NY), core, z, lax.rem(x + dx, NX))

    span = y * NCORE + core
    chord = z * NX + x

    def span_device(step):
        j = lax.rem(span + step + NY * NCORE, NY * NCORE)
        return (j // NCORE, lax.rem(j, NCORE), z, x)

    def chord_device(step):
        k = lax.rem(chord + step + NZ * NX, NZ * NX)
        return (y, core, k // NX, lax.rem(k, NX))

    partner = (y, 1 - core, z, x)
    beside = [span_device(1), span_device(-1), chord_device(1), chord_device(-1)]

    barrier = pltpu.get_barrier_semaphore()
    greeted = [line_device(*d) for d in line] + [plane_device(*d) for d in plane] + beside
    for device in greeted:
        pl.semaphore_signal(barrier, inc=1, device_id=device, device_id_type=MESH)

    own_ref[0] = jnp.concatenate(
        [ids_ref[...].astype(F32)] + [ctrl_ref[k : k + 1, :] for k in range(3)], axis=1
    )
    g1_ref[group * GROUP + place] = own_ref[0]
    table = jnp.concatenate(
        [shift_ref[...], speed_ref[...], jnp.zeros((2, shift_ref.shape[1]), F32)], axis=0
    )
    for k, part in enumerate(split3(table)):
        table_ref[k * 32 : (k + 1) * 32, :] = part

    pl.semaphore_wait(barrier, len(greeted))

    def first_copy(k, device):
        return pltpu.make_async_remote_copy(
            src_ref=own_ref,
            dst_ref=g1_ref.at[pl.ds(group * GROUP + place, 1)],
            send_sem=send1.at[k],
            recv_sem=recv1.at[k],
            device_id=device,
            device_id_type=MESH,
        )

    copies1 = [first_copy(k, line_device(*d)) for k, d in enumerate(line)]
    for copy in copies1:
        copy.start()
    for k, part in enumerate(split3(minv_ref[...])):
        m3_ref[k * 32 : (k + 1) * 32, :] = part
    ns_ref[...] = nodes_ref[...] * CROSS
    for copy in copies1:
        copy.wait_recv()

    def second_copy(k, device):
        rows = pl.ds(group * GROUP, GROUP)
        return pltpu.make_async_remote_copy(
            src_ref=g1_ref.at[rows],
            dst_ref=g1_ref.at[rows],
            send_sem=send2.at[k],
            recv_sem=recv2.at[k],
            device_id=device,
            device_id_type=MESH,
        )

    copies2 = [second_copy(k, plane_device(*d)) for k, d in enumerate(plane)]
    for copy in copies2:
        copy.start()
    for copy in copies1:
        copy.wait_send()
    for copy in copies2:
        copy.wait_recv()
    for copy in copies2:
        copy.wait_send()

    gp_ref[...] = g1_ref[...].reshape(DEVICES, 128)
    for ny in range(NY):
        idr_ref[ny * GROUP : (ny + 1) * GROUP, :] = jnp.concatenate(
            [gp_ref[(ny * NX + q) * GROUP : (ny * NX + q + 1) * GROUP, 0:32] for q in range(NX)],
            axis=1,
        )

    def selected(accs, parts_ref, index, blocks, which):
        spread = one_hot(index, blocks)
        for k in range(blocks // 2):
            pltpu.matmul_push_rhs(
                spread[k * 256 : (k + 1) * 256], staging_register=0, mxu_index=which % 2
            )
            pltpu.matmul_acc_lhs(
                accs[which], parts_ref[:, k * 256 : (k + 1) * 256], load_staged_rhs=0
            )

    def first_stage(*accs):
        for acc in accs:
            pltpu.matmul_pop(acc)

        def right_side(i, carry):
            for u in range(8):
                pair = idr_ref[pl.ds((i * 8 + u) * 2, 2), :]
                index = jnp.concatenate([pair[0:1], pair[1:2]], axis=1)
                selected(accs, table_ref, index, 8, u)
            for u in range(8):
                lanes = pl.ds(pl.multiple_of((i * 8 + u) * 256, 256), 256)
                r3_ref[:, lanes] = pltpu.matmul_pop(accs[u]).astype(BF16)
            return carry

        lax.fori_loop(0, 4, right_side, 0)

        for k in range(32):
            lanes = slice(k * 256, (k + 1) * 256)
            pltpu.matmul_push_rhs(
                jnp.concatenate([r3_ref[:, lanes], jnp.zeros((160, 256), BF16)], axis=0),
                staging_register=0,
                mxu_index=k % 2,
                transpose=True,
            )
            pltpu.matmul_acc_lhs(accs[k % 2], m3_ref[:, lanes], load_staged_rhs=0)
        cross_ref[...] = pltpu.matmul_pop(accs[0]) + pltpu.matmul_pop(accs[1])

    pl.run_scoped(first_stage, *[pltpu.ACC(u % 2)((96, 256), F32) for u in range(8)])
    cross = cross_ref[...]

    def piece(a, b):
        return cross[a * 32 : (a + 1) * 32, b * 32 : (b + 1) * 32]

    weights = piece(0, 0) + (
        (piece(0, 1) + piece(1, 0)) + (piece(1, 1) + (piece(0, 2) + piece(2, 0)))
    )
    wt_ref[:, 0:32] = weights
    mine = group * GROUP + place
    g2_ref[mine] = jnp.concatenate(
        [wt_ref[pl.ds(q, 8, stride=4), 0:32] for q in range(4)], axis=1
    )

    def third_copy(k, device):
        return pltpu.make_async_remote_copy(
            src_ref=g2_ref.at[pl.ds(mine, 1)],
            dst_ref=g2_ref.at[pl.ds(mine, 1)],
            send_sem=send3.at[k],
            recv_sem=recv3.at[k],
            device_id=device,
            device_id_type=MESH,
        )

    copies3 = [third_copy(k, line_device(0, k + 1)) for k in range(NZ - 1)]
    for copy in copies3:
        copy.start()

    def columns(l, target):
        for k in range(3):
            column = jnp.full((DEVICES, 128), 32 * (k + 1), jnp.int32) + l
            target[k] = jnp.take_along_axis(
                gp_ref[...], column, axis=1, mode="promise_in_bounds"
            )

    def tile(source, start):
        highs, lows = [], []
        for h in range(2):
            lanes = pl.ds(start + h * 128, 128)
            power = (
                source[0] * ns_ref[0:1, lanes]
                + source[1] * ns_ref[1:2, lanes]
                + source[2] * ns_ref[2:3, lanes]
            )
            value = jnp.exp2(power)
            high = value.astype(BF16)
            highs.append(high)
            lows.append((value - high.astype(F32)).astype(BF16))
        return jnp.concatenate(highs, axis=1), jnp.concatenate(lows, axis=1)

    def generate(l, source):
        def step(i, carry):
            for u in range(2):
                t = i * 2 + u
                high, low = tile(source, pl.multiple_of(t * 256, 256))
                kh_ref[l, t] = high
                kl_ref[l, t] = low
            return carry

        lax.fori_loop(0, TILES // 2, step, 0)

    def generate_range(first, last):
        def step(i, carry):
            l = i * 2
            columns(l, cb0_ref)
            generate(l, cb0_ref)
            columns(l + 1, cb1_ref)
            generate(l + 1, cb1_ref)
            return carry

        lax.fori_loop(first // 2, last // 2, step, 0)

    generate_range(0, 6)
    for copy in copies3:
        copy.wait_recv()

    def block_rows(of_y, of_x, of_core):
        return pl.ds((of_y * NX + of_x) * GROUP + of_core * NZ, NZ)

    def fourth_copy(k, device):
        rows = block_rows(y, x, core)
        return pltpu.make_async_remote_copy(
            src_ref=g2_ref.at[rows],
            dst_ref=g2_ref.at[rows],
            send_sem=send4.at[k],
            recv_sem=recv4.at[k],
            device_id=device,
            device_id_type=MESH,
        )

    copies4 = [fourth_copy(k, plane_device(*d)) for k, d in enumerate(plane)]
    for copy in copies4:
        copy.start()

    def fifth_copy(k, dy, dx):
        rows = block_rows(lax.rem(y + NY - dy, NY), lax.rem(x + NX - dx, NX), core)
        return pltpu.make_async_remote_copy(
            src_ref=g2_ref.at[rows],
            dst_ref=g2_ref.at[rows],
            send_sem=send5.at[k],
            recv_sem=recv5.at[k],
            device_id=partner,
            device_id_type=MESH,
        )

    copies5 = [fifth_copy(k, *d) for k, d in enumerate([(0, 0)] + plane)]
    copies5[0].start()
    for copy in copies3:
        copy.wait_send()
    generate_range(6, 16)
    for k in range(len(plane)):
        copies4[k].wait_recv()
        copies5[k + 1].start()
    for copy in copies4:
        copy.wait_send()
    turned = gp_ref[...].T
    scale_ref[...] = jnp.exp(
        -HALF_INV * (turned[32:64] ** 2 + turned[64:96] ** 2 + turned[96:128] ** 2)
    )
    generate_range(16, STORED)
    for copy in copies5:
        copy.wait_recv()
    for copy in copies5:
        copy.wait_send()

    for j in range(8):
        block = g2_ref[:, j, :].T
        for q in range(4):
            l = 4 * j + q
            value = block[q * 32 : (q + 1) * 32] * scale_ref[l : l + 1, :]
            high = value.astype(BF16)
            wc_ref[l, 0:32, :] = high
            wc_ref[l, 32:64, :] = (value - high.astype(F32)).astype(BF16)

    def products(highs, lows):
        for a, b in zip(highs, lows):
            pltpu.matmul_pop(a)
            pltpu.matmul_pop(b)

        def add(l, t, high, low):
            pltpu.matmul_push_rhs(high, staging_register=0, mxu_index=0)
            pltpu.matmul_acc_lhs(highs[t], wc_ref[l], load_staged_rhs=0)
            pltpu.matmul_push_rhs(low, staging_register=0, mxu_index=1)
            pltpu.matmul_acc_lhs(lows[t], wc_ref[l, 0:32], load_staged_rhs=0)

        def stored(l, carry):
            for t in range(TILES):
                add(l, t, kh_ref[l, t], kl_ref[l, t])
            return carry

        lax.fori_loop(0, STORED, stored, 0)

        def fresh(i, carry):
            for u, buffer in enumerate((cb0_ref, cb1_ref)):
                l = i * 2 + u
                columns(l, buffer)
                for t in range(TILES):
                    add(l, t, *tile(buffer, t * 256))
            return carry

        lax.fori_loop(STORED // 2, 16, fresh, 0)
        for t in range(TILES):
            lanes = slice(t * 256, (t + 1) * 256)
            first = pltpu.matmul_pop(highs[t])
            total = first[0:32] + first[32:64] + pltpu.matmul_pop(lows[t])
            place_of = nodes_ref[:, lanes]
            factor = jnp.exp(-HALF_INV * jnp.sum(place_of * place_of, axis=0, keepdims=True))
            base = jnp.concatenate([place_of] * 5 + [jnp.zeros((17, 256), F32)], axis=0)
            for k, part in enumerate(split3(total * factor + base)):
                t3_ref[k * 32 : (k + 1) * 32, lanes] = part

    pl.run_scoped(
        products,
        tuple(pltpu.ACC(0)((64, 256), F32) for _ in range(TILES)),
        tuple(pltpu.ACC(1)((32, 256), F32) for _ in range(TILES)),
    )

    def last_stage(*accs):
        for acc in accs:
            pltpu.matmul_pop(acc)

        def gather(i, carry):
            for u in range(8):
                pair = conn_ref[pl.ds((i * 8 + u) * 2, 2), :].astype(F32)
                index = jnp.concatenate([pair[0:1], pair[1:2]], axis=1)
                selected(accs, t3_ref, index, 16, u)
            for u in range(8):
                parts = pltpu.matmul_pop(accs[u])
                value = parts[0:32] + parts[32:64] + parts[64:96]
                first = (i * 8 + u) * 64
                gat_ref[pl.ds(first, 32), :] = value[:, 0:128]
                gat_ref[pl.ds(first + 32, 32), :] = value[:, 128:256]
            return carry

        lax.fori_loop(0, 4, gather, 0)

    pl.run_scoped(last_stage, *[pltpu.ACC(u % 2)((96, 256), F32) for u in range(8)])

    derivative = lobatto_derivative()

    def rows(first, p):
        return gat_ref[pl.ds(p * 32 + first, 5, stride=3), :]

    def metrics(p):
        a, b, c = p // 16, (p // 4) % 4, p % 4
        lines = (
            (a, [k * 16 + b * 4 + c for k in range(4)]),
            (b, [a * 16 + k * 4 + c for k in range(4)]),
            (c, [a * 16 + b * 4 + k for k in range(4)]),
        )
        jac = [[None] * 3 for _ in range(3)]
        for i in range(3):
            for d, (at, points) in enumerate(lines):
                terms = [
                    float(derivative[at, k]) * rows(i, q)
                    for k, q in enumerate(points)
                    if derivative[at, k] != 0.0
                ]
                jac[i][d] = functools.reduce(jnp.add, terms)

        def metric(d, i):
            i1, i2, d1, d2 = (i + 1) % 3, (i + 2) % 3, (d + 1) % 3, (d + 2) % 3
            return jac[i1][d1] * jac[i2][d2] - jac[i1][d2] * jac[i2][d1]

        speed = [rows(15 + i, p) for i in range(3)]
        entries = [[metric(d, i) for i in range(3)] for d in range(3)]
        det = (
            jac[0][0] * entries[0][0] + jac[0][1] * entries[1][0] + jac[0][2] * entries[2][0]
        )
        det_ref[:, p, :] = det
        for d in range(3):
            value = (
                entries[d][0] * speed[0] + entries[d][1] * speed[1] + entries[d][2] * speed[2]
            )
            flux_ref[:, d, p, :] = value
            if d > 0:
                fl_ref[d - 1, p, 0:5, :] = value

    fl_ref[...] = jnp.zeros_like(fl_ref)
    for p in range(64):
        metrics(p)

    lane = lax.broadcasted_iota(jnp.int32, (8, 128), 1)

    def quarters(values):
        out = values[0]
        for q in range(1, 4):
            out = jnp.where(lane >= q * 32, values[q], out)
        return out

    for t in range(4):
        index = jnp.broadcast_to(
            jnp.concatenate([elem_ref[t : t + 1, :]] * 4, axis=1), (8, 128)
        )
        for a in range(4):
            if t < 2:
                points = [a * 16 + q * 4 + 3 * t for q in range(4)]
            else:
                points = [a * 16 + 12 * (t - 2) + q for q in range(4)]
            picked = quarters(
                [
                    jnp.take_along_axis(
                        fl_ref[1 - t // 2, p], index, axis=1, mode="promise_in_bounds"
                    )
                    for p in points
                ]
            )
            tr_ref[t, a] = picked if t % 2 else -picked

    across = [(0, beside[1], 1), (1, beside[0], 0), (2, beside[3], 3), (3, beside[2], 2)]
    copies6 = [
        pltpu.make_async_remote_copy(
            src_ref=tr_ref.at[t],
            dst_ref=rc_ref.at[slot],
            send_sem=send6.at[t],
            recv_sem=recv6.at[slot],
            device_id=device,
            device_id_type=MESH,
        )
        for t, device, slot in across
    ]
    for copy in copies6:
        copy.start()
    for copy in copies6:
        copy.wait_recv()
    for copy in copies6:
        copy.wait_send()

    for t in range(4):
        index = jnp.broadcast_to(
            jnp.concatenate([match_ref[t : t + 1, :] + 32 * q for q in range(4)], axis=1), (8, 128)
        )
        for a in range(4):
            own = tr_ref[t, a]
            other = jnp.take_along_axis(rc_ref[t, a], index, axis=1, mode="promise_in_bounds")
            if t == 0:
                other = jnp.where(jnp.broadcast_to(span == 0, (8, 128)), -own, other)
            if t == 1:
                other = jnp.where(
                    jnp.broadcast_to(span == NY * NCORE - 1, (8, 128)), -own, other
                )
            value = 0.5 * (own - other)
            for q in range(4):
                face_ref[t, :, a * 4 + q, :] = value[0:5, q * 32 : (q + 1) * 32]


def on_device(
    node_pos, ctrl_pos, ctrl_ids, wing_shift, wing_speed, minv, conn, face_elem, face_match
):
    vmem = pl.BlockSpec(memory_space=pltpu.VMEM)
    dma = pltpu.SemaphoreType.DMA
    det, flux, face = pl.pallas_call(
        kernel,
        out_shape=(
            jax.ShapeDtypeStruct((5, 64, 128), F32),
            jax.ShapeDtypeStruct((5, 3, 64, 128), F32),
            jax.ShapeDtypeStruct((4, 5, 16, 32), F32),
        ),
        in_specs=[vmem] * 9,
        out_specs=[vmem] * 3,
        scratch_shapes=[
            pltpu.VMEM((1, 1, 128), F32),
            pltpu.VMEM((DEVICES, 1, 128), F32),
            pltpu.VMEM((DEVICES, 8, 128), F32),
            pltpu.VMEM((DEVICES, 128), F32),
            pltpu.VMEM((64, 128), F32),
            pltpu.VMEM((96, 1024), BF16),
            pltpu.VMEM((96, 8192), BF16),
            pltpu.VMEM((96, 8192), BF16),
            pltpu.VMEM((96, 256), F32),
            pltpu.VMEM((32, 128), F32),
            pltpu.VMEM((32, DEVICES), F32),
            pltpu.VMEM((32, 64, DEVICES), BF16),
            pltpu.VMEM((STORED, TILES, 256, 256), BF16),
            pltpu.VMEM((STORED, TILES, 256, 256), BF16),
            pltpu.VMEM((3, DEVICES, 128), F32),
            pltpu.VMEM((3, DEVICES, 128), F32),
            pltpu.VMEM((3, 2048), F32),
            pltpu.VMEM((96, 2048), BF16),
            pltpu.VMEM((64 * 32, 128), F32),
            pltpu.VMEM((2, 64, 8, 128), F32),
            pltpu.VMEM((4, 4, 8, 128), F32),
            pltpu.VMEM((4, 4, 8, 128), F32),
            dma((15,)),
            dma((15,)),
            dma((15,)),
            dma((15,)),
            dma((7,)),
            dma((7,)),
            dma((15,)),
            dma((15,)),
            dma((16,)),
            dma((16,)),
            dma((4,)),
            dma((4,)),
        ],
        compiler_params=pltpu.CompilerParams(
            collective_id=0, has_side_effects=True, vmem_limit_bytes=66 * 1000 * 1000
        ),
        name="wing",
    )(
        ctrl_ids.reshape(1, 32),
        ctrl_pos,
        node_pos,
        wing_shift,
        wing_speed,
        minv,
        conn,
        face_elem.reshape(4, 32),
        face_match.reshape(4, 32),
    )
    return det, flux, face.reshape(1, 1, 4, 5, 16, 32)


def solution(mesh):
    split = Mesh(mesh.devices.reshape(NY, NCORE, NZ, NX), SPAN_CHORD)
    return jax.shard_map(
        on_device,
        mesh=split,
        in_specs=(
            P(None, SPAN_CHORD),
            P(None, SPAN_CHORD),
            P(SPAN_CHORD),
            P(),
            P(),
            P(SPAN_CHORD, None),
            P(None, SPAN_CHORD),
            P(SPAN, CHORD, None, None),
            P(SPAN, CHORD, None, None),
        ),
        out_specs=(
            P(None, None, SPAN_CHORD),
            P(None, None, None, SPAN_CHORD),
            P(SPAN, CHORD, None, None, None, None),
        ),
        check_vma=False,
    )
```

```python
import functools

import jax
import jax.numpy as jnp
import numpy as np
from jax import lax
from jax.experimental import pallas as pl
from jax.experimental.pallas import tpu as pltpu
from jax.sharding import Mesh
from jax.sharding import PartitionSpec as P

SPAN_CHORD = ("y", "core", "z", "x")
SPAN = ("y", "core")
CHORD = ("z", "x")
NY, NCORE, NZ, NX = 4, 2, 8, 4
DEVICES = NY * NCORE * NZ * NX
GROUP = NCORE * NZ
MESH = pl.DeviceIdType.MESH
F32 = jnp.float32
BF16 = jnp.bfloat16

WIDTH = 0.1
HALF_INV = 1.0 / (2.0 * WIDTH**2)
CROSS = float(2.0 * HALF_INV * np.log2(np.e))
STORED = 24
TILES = 8


PAIRS = ((0, 0), (0, 1), (0, 2), (1, 0), (1, 1), (2, 0))


def selection():
    chosen = np.zeros((4, 512, 256), np.float32)
    for g in range(4):
        for l in range(8):
            for j, (part, _) in enumerate(PAIRS):
                for k in range(3):
                    chosen[g, part * 128 + 32 * (k + 1) + 8 * g + l, l * 32 + 3 * j + k] = 1.0
    return jnp.asarray(chosen, BF16)


def lobatto_derivative():
    points = np.array([-1.0, -1.0 / np.sqrt(5.0), 1.0 / np.sqrt(5.0), 1.0])
    barycentric = np.array(
        [
            1.0 / np.prod([points[t] - points[s] for s in range(4) if s != t])
            for t in range(4)
        ]
    )
    derivative = np.zeros((4, 4))
    for t in range(4):
        for s in range(4):
            if s != t:
                derivative[t, s] = barycentric[s] / barycentric[t] / (points[t] - points[s])
        derivative[t, t] = -np.sum(derivative[t])
    return derivative


def split3(value):
    high = value.astype(BF16)
    rest = value - high.astype(F32)
    middle = rest.astype(BF16)
    low = (rest - middle.astype(F32)).astype(BF16)
    return high, middle, low


def one_hot(index, blocks):
    width = index.shape[1]
    block = jnp.floor(index * (1.0 / 128.0))
    lane = (index - block * 128.0).astype(BF16)
    block = jnp.broadcast_to(block.astype(BF16), (128, width))
    row = lax.broadcasted_iota(jnp.int32, (128, width), 0).astype(F32).astype(BF16)
    one = jnp.ones((128, width), BF16)
    zero = jnp.zeros((128, width), BF16)
    inner = jnp.where(row == jnp.broadcast_to(lane, (128, width)), one, zero)
    return jnp.concatenate(
        [jnp.where(block == jnp.full((128, width), b, BF16), inner, zero) for b in range(blocks)],
        axis=0,
    )


def kernel(
    ids_in,
    ctrl_in,
    nodes_in,
    shift_in,
    speed_in,
    minv_in,
    conn_in,
    elem_in,
    match_in,
    sel_in,
    det_out,
    flux_out,
    face_ref,
    ids_ref,
    ctrl_ref,
    nodes_ref,
    shift_ref,
    speed_ref,
    minv_ref,
    conn_ref,
    elem_ref,
    match_ref,
    sel_ref,
    det_ref,
    flux_ref,
    own_ref,
    g1_ref,
    g2_ref,
    gp_ref,
    idr_ref,
    table_ref,
    r3_ref,
    m3_ref,
    cross_ref,
    wt_ref,
    scale_ref,
    wc_ref,
    kh_ref,
    kl_ref,
    parts_ref,
    lhs_ref,
    nb_ref,
    t3_ref,
    gat_ref,
    fl_ref,
    tr_ref,
    rc_ref,
    send1,
    recv1,
    send2,
    recv2,
    send3,
    recv3,
    send4,
    recv4,
    send5,
    recv5,
    send6,
    recv6,
    load,
    store,
):
    y, core, z, x = (lax.axis_index(name) for name in SPAN_CHORD)
    group = y * NX + x
    place = core * NZ + z
    line = [(dc, dz) for dc in range(NCORE) for dz in range(NZ) if (dc, dz) != (0, 0)]
    plane = [(dy, dx) for dy in range(NY) for dx in range(NX) if (dy, dx) != (0, 0)]

    def line_device(dc, dz):
        return (y, lax.rem(core + dc, NCORE), lax.rem(z + dz, NZ), x)

    def plane_device(dy, dx):
        return (lax.rem(y + dy, NY), core, z, lax.rem(x + dx, NX))

    span = y * NCORE + core
    chord = z * NX + x

    def span_device(step):
        j = lax.rem(span + step + NY * NCORE, NY * NCORE)
        return (j // NCORE, lax.rem(j, NCORE), z, x)

    def chord_device(step):
        k = lax.rem(chord + step + NZ * NX, NZ * NX)
        return (y, core, k // NX, lax.rem(k, NX))

    partner = (y, 1 - core, z, x)
    beside = [span_device(1), span_device(-1), chord_device(1), chord_device(-1)]

    barrier = pltpu.get_barrier_semaphore()
    greeted = [line_device(*d) for d in line] + [plane_device(*d) for d in plane] + beside
    for device in greeted:
        pl.semaphore_signal(barrier, inc=1, device_id=device, device_id_type=MESH)

    loads = [
        pltpu.make_async_copy(source, target, load.at[k])
        for k, (source, target) in enumerate(
            (
                (ids_in, ids_ref),
                (ctrl_in, ctrl_ref),
                (shift_in, shift_ref),
                (speed_in, speed_ref),
                (minv_in, minv_ref),
                (nodes_in, nodes_ref),
                (conn_in, conn_ref),
                (elem_in, elem_ref),
                (match_in, match_ref),
                (sel_in, sel_ref),
            )
        )
    ]
    for copy in loads:
        copy.start()
    for copy in loads[:4]:
        copy.wait()
    own_ref[0] = jnp.concatenate(
        [ids_ref[...].astype(F32)] + [ctrl_ref[k : k + 1, :] for k in range(3)], axis=1
    )
    g1_ref[group * GROUP + place] = own_ref[0]
    table = jnp.concatenate(
        [shift_ref[...], speed_ref[...], jnp.zeros((2, shift_ref.shape[1]), F32)], axis=0
    )
    for k, part in enumerate(split3(table)):
        table_ref[k * 32 : (k + 1) * 32, :] = part

    pl.semaphore_wait(barrier, len(greeted))

    def first_copy(k, device):
        return pltpu.make_async_remote_copy(
            src_ref=own_ref,
            dst_ref=g1_ref.at[pl.ds(group * GROUP + place, 1)],
            send_sem=send1.at[k],
            recv_sem=recv1.at[k],
            device_id=device,
            device_id_type=MESH,
        )

    copies1 = [first_copy(k, line_device(*d)) for k, d in enumerate(line)]
    for copy in copies1:
        copy.start()
    for copy in loads[4:]:
        copy.wait()
    for k, part in enumerate(split3(minv_ref[...])):
        m3_ref[k * 32 : (k + 1) * 32, :] = part
    node_parts = split3(nodes_ref[...] * CROSS)
    nb_ref[...] = jnp.concatenate(
        [node_parts[part].astype(F32) for _, part in PAIRS] + [jnp.zeros((14, 2048), F32)], axis=0
    ).astype(BF16)
    for copy in copies1:
        copy.wait_recv()

    def second_copy(k, device):
        rows = pl.ds(group * GROUP, GROUP)
        return pltpu.make_async_remote_copy(
            src_ref=g1_ref.at[rows],
            dst_ref=g1_ref.at[rows],
            send_sem=send2.at[k],
            recv_sem=recv2.at[k],
            device_id=device,
            device_id_type=MESH,
        )

    copies2 = [second_copy(k, plane_device(*d)) for k, d in enumerate(plane)]
    for copy in copies2:
        copy.start()
    for copy in copies1:
        copy.wait_send()
    for copy in copies2:
        copy.wait_recv()
    for copy in copies2:
        copy.wait_send()

    gp_ref[...] = g1_ref[...].reshape(DEVICES, 128)
    for ny in range(NY):
        idr_ref[ny * GROUP : (ny + 1) * GROUP, :] = jnp.concatenate(
            [gp_ref[(ny * NX + q) * GROUP : (ny * NX + q + 1) * GROUP, 0:32] for q in range(NX)],
            axis=1,
        )

    def selected(accs, parts_ref, index, blocks, which):
        spread = one_hot(index, blocks)
        for k in range(blocks // 2):
            pltpu.matmul_push_rhs(
                spread[k * 256 : (k + 1) * 256], staging_register=0, mxu_index=which % 2
            )
            pltpu.matmul_acc_lhs(
                accs[which], parts_ref[:, k * 256 : (k + 1) * 256], load_staged_rhs=0
            )

    def first_stage(*accs):
        for acc in accs:
            pltpu.matmul_pop(acc)

        def right_side(i, carry):
            for u in range(8):
                pair = idr_ref[pl.ds((i * 8 + u) * 2, 2), :]
                index = jnp.concatenate([pair[0:1], pair[1:2]], axis=1)
                selected(accs, table_ref, index, 8, u)
            for u in range(8):
                lanes = pl.ds(pl.multiple_of((i * 8 + u) * 256, 256), 256)
                r3_ref[:, lanes] = pltpu.matmul_pop(accs[u]).astype(BF16)
            return carry

        lax.fori_loop(0, 4, right_side, 0)

        for k in range(32):
            lanes = slice(k * 256, (k + 1) * 256)
            pltpu.matmul_push_rhs(
                jnp.concatenate([r3_ref[:, lanes], jnp.zeros((160, 256), BF16)], axis=0),
                staging_register=0,
                mxu_index=k % 2,
                transpose=True,
            )
            pltpu.matmul_acc_lhs(accs[k % 2], m3_ref[:, lanes], load_staged_rhs=0)
        cross_ref[...] = pltpu.matmul_pop(accs[0]) + pltpu.matmul_pop(accs[1])

    pl.run_scoped(first_stage, *[pltpu.ACC(u % 2)((96, 256), F32) for u in range(8)])
    cross = cross_ref[...]

    def piece(a, b):
        return cross[a * 32 : (a + 1) * 32, b * 32 : (b + 1) * 32]

    weights = piece(0, 0) + (
        (piece(0, 1) + piece(1, 0)) + (piece(1, 1) + (piece(0, 2) + piece(2, 0)))
    )
    wt_ref[:, 0:32] = weights
    mine = group * GROUP + place
    g2_ref[mine] = jnp.concatenate(
        [wt_ref[pl.ds(q, 8, stride=4), 0:32] for q in range(4)], axis=1
    )

    def third_copy(k, device):
        return pltpu.make_async_remote_copy(
            src_ref=g2_ref.at[pl.ds(mine, 1)],
            dst_ref=g2_ref.at[pl.ds(mine, 1)],
            send_sem=send3.at[k],
            recv_sem=recv3.at[k],
            device_id=device,
            device_id_type=MESH,
        )

    copies3 = [third_copy(k, line_device(0, k + 1)) for k in range(NZ - 1)]
    for copy in copies3:
        copy.start()

    def weights_of(power):
        value = jnp.exp2(power)
        high = value.astype(BF16)
        return high, (value - high.astype(F32)).astype(BF16)

    def cross_rhs(l, lanes):
        pieces = [nb_ref[:, lanes]]
        if l > 0:
            pieces = [jnp.zeros((32 * l, 256), BF16)] + pieces
        if l < 7:
            pieces = pieces + [jnp.zeros((32 * (7 - l), 256), BF16)]
        return jnp.concatenate(pieces, axis=0)

    def generate(accs):
        def step(t, carry):
            lanes = pl.ds(pl.multiple_of(t * 256, 256), 256)
            for l in range(8):
                pltpu.matmul_push_rhs(cross_rhs(l, lanes), staging_register=0, mxu_index=l % 2)
                for g in range(3):
                    pltpu.matmul_acc_lhs(
                        accs[l % 2][g], lhs_ref[g], load_staged_rhs=0 if g == 0 else None
                    )
                for g in range(3):
                    high, low = weights_of(pltpu.matmul_pop(accs[l % 2][g]))
                    kh_ref[g * 8 + l, t] = high
                    kl_ref[g * 8 + l, t] = low
            return carry

        return step

    def start_generation(*accs):
        for acc in accs:
            pltpu.matmul_pop(acc)
        for g in range(4):
            for k in range(2):
                pltpu.matmul_push_rhs(
                    sel_ref[g, k * 256 : (k + 1) * 256, :], staging_register=0, mxu_index=g % 2
                )
                pltpu.matmul_acc_lhs(accs[g], parts_ref[k], load_staged_rhs=0)
        for g in range(4):
            lhs_ref[g] = pltpu.matmul_pop(accs[g]).astype(BF16)

    def generate_range(first, last):
        def scoped(zero, one):
            for acc in (*zero, *one):
                pltpu.matmul_pop(acc)
            lax.fori_loop(first, last, generate((zero, one)), 0)

        pl.run_scoped(
            scoped,
            tuple(pltpu.ACC(0)((256, 256), F32) for _ in range(3)),
            tuple(pltpu.ACC(1)((256, 256), F32) for _ in range(3)),
        )

    for k, part in enumerate(split3(gp_ref[...])):
        parts_ref[k // 2, :, (k % 2) * 128 : (k % 2 + 1) * 128] = part
    parts_ref[1, :, 128:256] = jnp.zeros((DEVICES, 128), BF16)
    pl.run_scoped(start_generation, *[pltpu.ACC(g % 2)((256, 256), F32) for g in range(4)])

    generate_range(0, 3)
    for copy in copies3:
        copy.wait_recv()

    def block_rows(of_y, of_x, of_core):
        return pl.ds((of_y * NX + of_x) * GROUP + of_core * NZ, NZ)

    def fourth_copy(k, device):
        rows = block_rows(y, x, core)
        return pltpu.make_async_remote_copy(
            src_ref=g2_ref.at[rows],
            dst_ref=g2_ref.at[rows],
            send_sem=send4.at[k],
            recv_sem=recv4.at[k],
            device_id=device,
            device_id_type=MESH,
        )

    copies4 = [fourth_copy(k, plane_device(*d)) for k, d in enumerate(plane)]
    for copy in copies4:
        copy.start()

    def fifth_copy(k, dy, dx):
        rows = block_rows(lax.rem(y + NY - dy, NY), lax.rem(x + NX - dx, NX), core)
        return pltpu.make_async_remote_copy(
            src_ref=g2_ref.at[rows],
            dst_ref=g2_ref.at[rows],
            send_sem=send5.at[k],
            recv_sem=recv5.at[k],
            device_id=partner,
            device_id_type=MESH,
        )

    copies5 = [fifth_copy(k, *d) for k, d in enumerate([(0, 0)] + plane)]
    copies5[0].start()
    for copy in copies3:
        copy.wait_send()
    generate_range(3, 8)
    for k in range(len(plane)):
        copies4[k].wait_recv()
        copies5[k + 1].start()
    for copy in copies4:
        copy.wait_send()
    turned = gp_ref[...].T
    scale_ref[...] = jnp.exp(
        -HALF_INV * (turned[32:64] ** 2 + turned[64:96] ** 2 + turned[96:128] ** 2)
    )
    for copy in copies5:
        copy.wait_recv()
    for copy in copies5:
        copy.wait_send()

    for j in range(8):
        block = g2_ref[:, j, :].T
        for q in range(4):
            l = 4 * j + q
            value = block[q * 32 : (q + 1) * 32] * scale_ref[l : l + 1, :]
            high = value.astype(BF16)
            wc_ref[l, 0:32, :] = high
            wc_ref[l, 32:64, :] = (value - high.astype(F32)).astype(BF16)

    def products(zero, one, high_acc, low_acc):
        accs = (zero, one)
        for acc in (*zero, *one, high_acc, low_acc):
            pltpu.matmul_pop(acc)

        def add(l, high, low):
            pltpu.matmul_push_rhs(high, staging_register=0, mxu_index=0)
            pltpu.matmul_acc_lhs(high_acc, wc_ref[l], load_staged_rhs=0)
            pltpu.matmul_push_rhs(low, staging_register=0, mxu_index=1)
            pltpu.matmul_acc_lhs(low_acc, wc_ref[l, 0:32], load_staged_rhs=0)

        def columns(t, carry):
            lanes = pl.ds(pl.multiple_of(t * 256, 256), 256)

            def power(l):
                pltpu.matmul_push_rhs(cross_rhs(l, lanes), staging_register=1, mxu_index=l % 2)
                pltpu.matmul_acc_lhs(accs[l % 2][(l // 2) % 2], lhs_ref[3], load_staged_rhs=1)

            power(0)
            power(1)
            for l in range(8):
                high, low = weights_of(pltpu.matmul_pop(accs[l % 2][(l // 2) % 2]))
                if l < 6:
                    power(l + 2)
                for k in range(3 * l, 3 * l + 3):
                    add(k, kh_ref[k, t], kl_ref[k, t])
                add(24 + l, high, low)
            first = pltpu.matmul_pop(high_acc)
            total = first[0:32] + first[32:64] + pltpu.matmul_pop(low_acc)
            place_of = nodes_ref[:, lanes]
            factor = jnp.exp(-HALF_INV * jnp.sum(place_of * place_of, axis=0, keepdims=True))
            base = jnp.concatenate([place_of] * 5 + [jnp.zeros((17, 256), F32)], axis=0)
            for k, part in enumerate(split3(total * factor + base)):
                t3_ref[k * 32 : (k + 1) * 32, lanes] = part
            return carry

        lax.fori_loop(0, TILES, columns, 0)

    pl.run_scoped(
        products,
        tuple(pltpu.ACC(0)((256, 256), F32) for _ in range(2)),
        tuple(pltpu.ACC(1)((256, 256), F32) for _ in range(2)),
        pltpu.ACC(0)((64, 256), F32),
        pltpu.ACC(1)((32, 256), F32),
    )

    def last_stage(*accs):
        for acc in accs:
            pltpu.matmul_pop(acc)

        def gather(i, carry):
            for u in range(8):
                pair = conn_ref[pl.ds((i * 8 + u) * 2, 2), :].astype(F32)
                index = jnp.concatenate([pair[0:1], pair[1:2]], axis=1)
                selected(accs, t3_ref, index, 16, u)
            for u in range(8):
                parts = pltpu.matmul_pop(accs[u])
                value = parts[0:32] + parts[32:64] + parts[64:96]
                first = (i * 8 + u) * 64
                gat_ref[pl.ds(first, 32), :] = value[:, 0:128]
                gat_ref[pl.ds(first + 32, 32), :] = value[:, 128:256]
            return carry

        lax.fori_loop(0, 4, gather, 0)

    pl.run_scoped(last_stage, *[pltpu.ACC(u % 2)((96, 256), F32) for u in range(8)])

    derivative = lobatto_derivative()

    def rows(first, p):
        return gat_ref[pl.ds(p * 32 + first, 5, stride=3), :]

    def jacobian(p, directions):
        a, b, c = p // 16, (p // 4) % 4, p % 4
        lines = (
            (a, [k * 16 + b * 4 + c for k in range(4)]),
            (b, [a * 16 + k * 4 + c for k in range(4)]),
            (c, [a * 16 + b * 4 + k for k in range(4)]),
        )
        jac = [[None] * 3 for _ in range(3)]
        for i in range(3):
            for d in directions:
                at, points = lines[d]
                terms = [
                    float(derivative[at, k]) * rows(i, q)
                    for k, q in enumerate(points)
                    if derivative[at, k] != 0.0
                ]
                jac[i][d] = functools.reduce(jnp.add, terms)
        return jac

    def metric(jac, d, i):
        i1, i2, d1, d2 = (i + 1) % 3, (i + 2) % 3, (d + 1) % 3, (d + 2) % 3
        return jac[i1][d1] * jac[i2][d2] - jac[i1][d2] * jac[i2][d1]

    def normal(entries, speed):
        return entries[0] * speed[0] + entries[1] * speed[1] + entries[2] * speed[2]

    def face_flux(p, d):
        jac = jacobian(p, [k for k in range(3) if k != d])
        speed = [rows(15 + i, p) for i in range(3)]
        fl_ref[d - 1, p, 0:5, :] = normal([metric(jac, d, i) for i in range(3)], speed)

    def metrics(p):
        jac = jacobian(p, range(3))
        speed = [rows(15 + i, p) for i in range(3)]
        entries = [[metric(jac, d, i) for i in range(3)] for d in range(3)]
        det_ref[:, p, :] = (
            jac[0][0] * entries[0][0] + jac[0][1] * entries[1][0] + jac[0][2] * entries[2][0]
        )
        for d in range(3):
            flux_ref[:, d, p, :] = normal(entries[d], speed)

    fl_ref[...] = jnp.zeros_like(fl_ref)
    for p in range(64):
        if p % 4 in (0, 3):
            face_flux(p, 2)
        if (p // 4) % 4 in (0, 3):
            face_flux(p, 1)

    lane = lax.broadcasted_iota(jnp.int32, (8, 128), 1)

    def quarters(values):
        out = values[0]
        for q in range(1, 4):
            out = jnp.where(lane >= q * 32, values[q], out)
        return out

    for t in range(4):
        index = jnp.broadcast_to(
            jnp.concatenate([elem_ref[t : t + 1, :]] * 4, axis=1), (8, 128)
        )
        for a in range(4):
            if t < 2:
                points = [a * 16 + q * 4 + 3 * t for q in range(4)]
            else:
                points = [a * 16 + 12 * (t - 2) + q for q in range(4)]
            picked = quarters(
                [
                    jnp.take_along_axis(
                        fl_ref[1 - t // 2, p], index, axis=1, mode="promise_in_bounds"
                    )
                    for p in points
                ]
            )
            tr_ref[t, a] = picked if t % 2 else -picked

    across = [(0, beside[1], 1), (1, beside[0], 0), (2, beside[3], 3), (3, beside[2], 2)]
    copies6 = [
        pltpu.make_async_remote_copy(
            src_ref=tr_ref.at[t],
            dst_ref=rc_ref.at[slot],
            send_sem=send6.at[t],
            recv_sem=recv6.at[slot],
            device_id=device,
            device_id_type=MESH,
        )
        for t, device, slot in across
    ]
    for copy in copies6:
        copy.start()
    for p in range(64):
        metrics(p)
    stores = [
        pltpu.make_async_copy(det_ref, det_out, store.at[0]),
        pltpu.make_async_copy(flux_ref, flux_out, store.at[1]),
    ]
    for copy in stores:
        copy.start()
    for copy in copies6:
        copy.wait_recv()
    for copy in copies6:
        copy.wait_send()

    for t in range(4):
        index = jnp.broadcast_to(
            jnp.concatenate([match_ref[t : t + 1, :] + 32 * q for q in range(4)], axis=1), (8, 128)
        )
        for a in range(4):
            own = tr_ref[t, a]
            other = jnp.take_along_axis(rc_ref[t, a], index, axis=1, mode="promise_in_bounds")
            if t == 0:
                other = jnp.where(jnp.broadcast_to(span == 0, (8, 128)), -own, other)
            if t == 1:
                other = jnp.where(
                    jnp.broadcast_to(span == NY * NCORE - 1, (8, 128)), -own, other
                )
            value = 0.5 * (own - other)
            for q in range(4):
                face_ref[t, :, a * 4 + q, :] = value[0:5, q * 32 : (q + 1) * 32]
    for copy in stores:
        copy.wait()


def on_device(
    node_pos, ctrl_pos, ctrl_ids, wing_shift, wing_speed, minv, conn, face_elem, face_match
):
    vmem = pl.BlockSpec(memory_space=pltpu.VMEM)
    hbm = pl.BlockSpec(memory_space=pltpu.HBM)
    dma = pltpu.SemaphoreType.DMA
    det, flux, face = pl.pallas_call(
        kernel,
        out_shape=(
            jax.ShapeDtypeStruct((5, 64, 128), F32),
            jax.ShapeDtypeStruct((5, 3, 64, 128), F32),
            jax.ShapeDtypeStruct((4, 5, 16, 32), F32),
        ),
        in_specs=[hbm] * 10,
        out_specs=[hbm, hbm, vmem],
        scratch_shapes=[
            pltpu.VMEM((1, 32), jnp.int32),
            pltpu.VMEM((3, 32), F32),
            pltpu.VMEM((3, 2048), F32),
            pltpu.VMEM((15, 1024), F32),
            pltpu.VMEM((15, 1024), F32),
            pltpu.VMEM((32, 8192), F32),
            pltpu.VMEM((64, 128), jnp.int32),
            pltpu.VMEM((4, 32), jnp.int32),
            pltpu.VMEM((4, 32), jnp.int32),
            pltpu.VMEM((4, 512, 256), BF16),
            pltpu.VMEM((5, 64, 128), F32),
            pltpu.VMEM((5, 3, 64, 128), F32),
            pltpu.VMEM((1, 1, 128), F32),
            pltpu.VMEM((DEVICES, 1, 128), F32),
            pltpu.VMEM((DEVICES, 8, 128), F32),
            pltpu.VMEM((DEVICES, 128), F32),
            pltpu.VMEM((64, 128), F32),
            pltpu.VMEM((96, 1024), BF16),
            pltpu.VMEM((96, 8192), BF16),
            pltpu.VMEM((96, 8192), BF16),
            pltpu.VMEM((96, 256), F32),
            pltpu.VMEM((32, 128), F32),
            pltpu.VMEM((32, DEVICES), F32),
            pltpu.VMEM((32, 64, DEVICES), BF16),
            pltpu.VMEM((STORED, TILES, 256, 256), BF16),
            pltpu.VMEM((STORED, TILES, 256, 256), BF16),
            pltpu.VMEM((2, DEVICES, 256), BF16),
            pltpu.VMEM((4, DEVICES, 256), BF16),
            pltpu.VMEM((32, 2048), BF16),
            pltpu.VMEM((96, 2048), BF16),
            pltpu.VMEM((64 * 32, 128), F32),
            pltpu.VMEM((2, 64, 8, 128), F32),
            pltpu.VMEM((4, 4, 8, 128), F32),
            pltpu.VMEM((4, 4, 8, 128), F32),
            dma((15,)),
            dma((15,)),
            dma((15,)),
            dma((15,)),
            dma((7,)),
            dma((7,)),
            dma((15,)),
            dma((15,)),
            dma((16,)),
            dma((16,)),
            dma((4,)),
            dma((4,)),
            dma((10,)),
            dma((2,)),
        ],
        compiler_params=pltpu.CompilerParams(
            collective_id=0, has_side_effects=True, vmem_limit_bytes=66 * 1000 * 1000
        ),
        name="wing",
    )(
        ctrl_ids.reshape(1, 32),
        ctrl_pos,
        node_pos,
        wing_shift,
        wing_speed,
        minv,
        conn,
        face_elem.reshape(4, 32),
        face_match.reshape(4, 32),
        selection(),
    )
    return det, flux, face.reshape(1, 1, 4, 5, 16, 32)


def solution(mesh):
    split = Mesh(mesh.devices.reshape(NY, NCORE, NZ, NX), SPAN_CHORD)
    return jax.shard_map(
        on_device,
        mesh=split,
        in_specs=(
            P(None, SPAN_CHORD),
            P(None, SPAN_CHORD),
            P(SPAN_CHORD),
            P(),
            P(),
            P(SPAN_CHORD, None),
            P(None, SPAN_CHORD),
            P(SPAN, CHORD, None, None),
            P(SPAN, CHORD, None, None),
        ),
        out_specs=(
            P(None, None, SPAN_CHORD),
            P(None, None, None, SPAN_CHORD),
            P(SPAN, CHORD, None, None, None, None),
        ),
        check_vma=False,
    )
```

```python
import functools

import jax
import jax.numpy as jnp
import numpy as np
from jax import lax
from jax.experimental import pallas as pl
from jax.experimental.pallas import tpu as pltpu
from jax.sharding import Mesh
from jax.sharding import PartitionSpec as P

SPAN_CHORD = ("y", "core", "z", "x")
SPAN = ("y", "core")
CHORD = ("z", "x")
NY, NCORE, NZ, NX = 4, 2, 8, 4
DEVICES = NY * NCORE * NZ * NX
GROUP = NCORE * NZ
MESH = pl.DeviceIdType.MESH
F32 = jnp.float32
BF16 = jnp.bfloat16

WIDTH = 0.1
HALF_INV = 1.0 / (2.0 * WIDTH**2)
CROSS = float(2.0 * HALF_INV * np.log2(np.e))
STORED = 24
TILES = 8
R_PERMUTED = 24
R_UNITS = (64 - R_PERMUTED) // 4


PAIRS = ((0, 0), (0, 1), (0, 2), (1, 0), (1, 1), (2, 0))


def selection():
    chosen = np.zeros((4, 384, 256), np.float32)
    for g in range(4):
        for l in range(8):
            for j, (part, _) in enumerate(PAIRS):
                for k in range(3):
                    chosen[g, part * 128 + 32 * (k + 1) + 8 * g + l, l * 32 + 3 * j + k] = 1.0
    return jnp.asarray(chosen, BF16)


def lobatto_derivative():
    points = np.array([-1.0, -1.0 / np.sqrt(5.0), 1.0 / np.sqrt(5.0), 1.0])
    barycentric = np.array(
        [
            1.0 / np.prod([points[t] - points[s] for s in range(4) if s != t])
            for t in range(4)
        ]
    )
    derivative = np.zeros((4, 4))
    for t in range(4):
        for s in range(4):
            if s != t:
                derivative[t, s] = barycentric[s] / barycentric[t] / (points[t] - points[s])
        derivative[t, t] = -np.sum(derivative[t])
    return derivative


def split3(value):
    high = value.astype(BF16)
    rest = value - high.astype(F32)
    middle = rest.astype(BF16)
    low = (rest - middle.astype(F32)).astype(BF16)
    return high, middle, low


def one_hot(index, blocks):
    width = index.shape[1]
    block = jnp.floor(index * (1.0 / 128.0))
    lane = (index - block * 128.0).astype(BF16)
    block = jnp.broadcast_to(block.astype(BF16), (128, width))
    row = lax.broadcasted_iota(jnp.int32, (128, width), 0).astype(F32).astype(BF16)
    one = jnp.ones((128, width), BF16)
    zero = jnp.zeros((128, width), BF16)
    inner = jnp.where(row == jnp.broadcast_to(lane, (128, width)), one, zero)
    return jnp.concatenate(
        [jnp.where(block == jnp.full((128, width), b, BF16), inner, zero) for b in range(blocks)],
        axis=0,
    )


def kernel(
    ids_in,
    ctrl_in,
    nodes_in,
    shift_in,
    speed_in,
    minv_in,
    conn_in,
    elem_in,
    match_in,
    sel_in,
    det_out,
    flux_out,
    face_ref,
    ids_ref,
    ctrl_ref,
    nodes_ref,
    shift_ref,
    speed_ref,
    minv_ref,
    conn_ref,
    elem_ref,
    match_ref,
    sel_ref,
    det_ref,
    flux_ref,
    own_ref,
    g1_ref,
    g2_ref,
    gp_ref,
    idr_ref,
    table_ref,
    plain_ref,
    r3_ref,
    m3_ref,
    cross_ref,
    wt_ref,
    scale_ref,
    wc_ref,
    kh_ref,
    kl_ref,
    parts_ref,
    lhs_ref,
    nb_ref,
    t3_ref,
    tab_ref,
    gat_ref,
    fl_ref,
    tr_ref,
    rc_ref,
    sems,
    recv3,
    load,
    store,
):
    y, core, z, x = (lax.axis_index(name) for name in SPAN_CHORD)
    group = y * NX + x
    place = core * NZ + z
    line = [(dc, dz) for dc in range(NCORE) for dz in range(NZ) if (dc, dz) != (0, 0)]
    plane = [(dy, dx) for dy in range(NY) for dx in range(NX) if (dy, dx) != (0, 0)]

    def line_device(dc, dz):
        return (y, lax.rem(core + dc, NCORE), lax.rem(z + dz, NZ), x)

    def plane_device(dy, dx):
        return (lax.rem(y + dy, NY), core, z, lax.rem(x + dx, NX))

    span = y * NCORE + core
    chord = z * NX + x

    def span_device(step):
        j = lax.rem(span + step + NY * NCORE, NY * NCORE)
        return (j // NCORE, lax.rem(j, NCORE), z, x)

    def chord_device(step):
        k = lax.rem(chord + step + NZ * NX, NZ * NX)
        return (y, core, k // NX, lax.rem(k, NX))

    partner = (y, 1 - core, z, x)
    beside = [span_device(1), span_device(-1), chord_device(1), chord_device(-1)]

    barrier = pltpu.get_barrier_semaphore()
    greeted = [line_device(*d) for d in line] + [plane_device(*d) for d in plane] + beside
    for device in greeted:
        pl.semaphore_signal(barrier, inc=1, device_id=device, device_id_type=MESH)

    loads = [
        pltpu.make_async_copy(source, target, load.at[k])
        for k, (source, target) in enumerate(
            (
                (ids_in, ids_ref),
                (ctrl_in, ctrl_ref),
                (shift_in, shift_ref),
                (speed_in, speed_ref),
                (minv_in, minv_ref),
                (nodes_in, nodes_ref),
                (conn_in, conn_ref),
                (elem_in, elem_ref),
                (match_in, match_ref),
                (sel_in, sel_ref),
            )
        )
    ]
    for copy in loads:
        copy.start()
    for copy in loads[:4]:
        copy.wait()
    own_ref[0] = jnp.concatenate(
        [ids_ref[...].astype(F32)] + [ctrl_ref[k : k + 1, :] for k in range(3)], axis=1
    )
    g1_ref[group * GROUP + place] = own_ref[0]
    table = jnp.concatenate(
        [shift_ref[...], speed_ref[...], jnp.zeros((2, shift_ref.shape[1]), F32)], axis=0
    )
    plain_ref[...] = table
    for k, part in enumerate(split3(table)):
        table_ref[k * 32 : (k + 1) * 32, :] = part

    pl.semaphore_wait(barrier, len(greeted))

    def first_copy(k, device):
        return pltpu.make_async_remote_copy(
            src_ref=own_ref,
            dst_ref=g1_ref.at[pl.ds(group * GROUP + place, 1)],
            send_sem=sems.at[0],
            recv_sem=sems.at[1],
            device_id=device,
            device_id_type=MESH,
        )

    copies1 = [first_copy(k, line_device(*d)) for k, d in enumerate(line)]
    for copy in copies1:
        copy.start()
    for copy in loads[4:]:
        copy.wait()
    for k, part in enumerate(split3(minv_ref[...])):
        m3_ref[k * 32 : (k + 1) * 32, :] = part
    node_parts = split3(nodes_ref[...] * CROSS)
    nb_ref[...] = jnp.concatenate(
        [node_parts[part].astype(F32) for _, part in PAIRS] + [jnp.zeros((14, 2048), F32)], axis=0
    ).astype(BF16)
    def all_rows(ref, count, sent, received):
        return pltpu.make_async_remote_copy(
            src_ref=ref.at[pl.ds(0, count)],
            dst_ref=ref.at[pl.ds(0, count)],
            send_sem=sems.at[sent],
            recv_sem=sems.at[received],
            device_id=partner,
            device_id_type=MESH,
        )

    every1 = all_rows(g1_ref, len(line), 0, 1)
    every2 = all_rows(g1_ref, len(plane) * GROUP, 2, 3)
    every1.wait_recv()

    def second_copy(k, device):
        rows = pl.ds(group * GROUP, GROUP)
        return pltpu.make_async_remote_copy(
            src_ref=g1_ref.at[rows],
            dst_ref=g1_ref.at[rows],
            send_sem=sems.at[2],
            recv_sem=sems.at[3],
            device_id=device,
            device_id_type=MESH,
        )

    copies2 = [second_copy(k, plane_device(*d)) for k, d in enumerate(plane)]
    for copy in copies2:
        copy.start()
    every1.wait_send()
    every2.wait_recv()
    every2.wait_send()

    gp_ref[...] = g1_ref[...].reshape(DEVICES, 128)
    for ny in range(NY):
        idr_ref[ny * GROUP : (ny + 1) * GROUP, :] = jnp.concatenate(
            [gp_ref[(ny * NX + q) * GROUP : (ny * NX + q + 1) * GROUP, 0:32] for q in range(NX)],
            axis=1,
        )

    def permuted(source_ref, index, blocks):
        node = jnp.broadcast_to(index, (8, 128))
        lane = node & 127
        block = node >> 7
        found = [None] * 4
        for k in range(blocks):
            here = block == k
            for r in range(4):
                taken = jnp.take_along_axis(
                    source_ref[r * 8 : r * 8 + 8, k * 128 : (k + 1) * 128],
                    lane,
                    axis=1,
                    mode="promise_in_bounds",
                )
                found[r] = taken if k == 0 else jnp.where(here, taken, found[r])
        return found

    def selected(accs, parts_ref, index, blocks, which):
        spread = one_hot(index, blocks)
        for k in range(blocks // 2):
            pltpu.matmul_push_rhs(
                spread[k * 256 : (k + 1) * 256], staging_register=0, mxu_index=which % 2
            )
            pltpu.matmul_acc_lhs(
                accs[which], parts_ref[:, k * 256 : (k + 1) * 256], load_staged_rhs=0
            )

    def first_stage(*accs):
        for acc in accs:
            pltpu.matmul_pop(acc)

        def right_side(i, carry):
            for u in range(R_UNITS):
                pair = idr_ref[pl.ds((i * R_UNITS + u) * 2, 2), :]
                index = jnp.concatenate([pair[0:1], pair[1:2]], axis=1)
                selected(accs, table_ref, index, 8, u)
            for v in range(R_PERMUTED // 2):
                row = 64 - R_PERMUTED + i * (R_PERMUTED // 2) + v
                lanes = pl.ds(pl.multiple_of(row * 128, 128), 128)
                found = permuted(plain_ref, idr_ref[pl.ds(row, 1), :].astype(jnp.int32), 8)
                for k, part in enumerate(split3(jnp.concatenate(found, axis=0))):
                    r3_ref[k * 32 : (k + 1) * 32, lanes] = part
            for u in range(R_UNITS):
                lanes = pl.ds(pl.multiple_of((i * R_UNITS + u) * 256, 256), 256)
                r3_ref[:, lanes] = pltpu.matmul_pop(accs[u]).astype(BF16)
            return carry

        lax.fori_loop(0, 2, right_side, 0)

        for k in range(32):
            lanes = slice(k * 256, (k + 1) * 256)
            pltpu.matmul_push_rhs(
                jnp.concatenate([r3_ref[:, lanes], jnp.zeros((160, 256), BF16)], axis=0),
                staging_register=0,
                mxu_index=k % 2,
                transpose=True,
            )
            pltpu.matmul_acc_lhs(accs[k % 2], m3_ref[:, lanes], load_staged_rhs=0)
        cross_ref[...] = pltpu.matmul_pop(accs[0]) + pltpu.matmul_pop(accs[1])

    pl.run_scoped(first_stage, *[pltpu.ACC(u % 2)((96, 256), F32) for u in range(R_UNITS)])
    cross = cross_ref[...]

    def piece(a, b):
        return cross[a * 32 : (a + 1) * 32, b * 32 : (b + 1) * 32]

    weights = piece(0, 0) + (
        (piece(0, 1) + piece(1, 0)) + (piece(1, 1) + (piece(0, 2) + piece(2, 0)))
    )
    wt_ref[:, 0:32] = weights
    mine = group * GROUP + place
    g2_ref[mine] = jnp.concatenate(
        [wt_ref[pl.ds(q, 8, stride=4), 0:32] for q in range(4)], axis=1
    )

    def third_copy(k, device):
        return pltpu.make_async_remote_copy(
            src_ref=g2_ref.at[pl.ds(mine, 1)],
            dst_ref=g2_ref.at[pl.ds(mine, 1)],
            send_sem=sems.at[4],
            recv_sem=recv3.at[k],
            device_id=device,
            device_id_type=MESH,
        )

    copies3 = [third_copy(k, line_device(0, k + 1)) for k in range(NZ - 1)]
    for copy in copies3:
        copy.start()

    def block_rows(of_y, of_x, of_core):
        return pl.ds((of_y * NX + of_x) * GROUP + of_core * NZ, NZ)

    def fourth_copy(k, device, rows):
        return pltpu.make_async_remote_copy(
            src_ref=g2_ref.at[rows],
            dst_ref=g2_ref.at[rows],
            send_sem=sems.at[5],
            recv_sem=sems.at[6],
            device_id=device,
            device_id_type=MESH,
        )

    def forward(step):
        row = group * GROUP + core * NZ + lax.rem(z + NZ - step, NZ)
        for k, d in enumerate(plane):
            fourth_copy(k, plane_device(*d), pl.ds(row, 1)).start()

    forward(0)

    def parts_of(value):
        high = value.astype(BF16)
        return high, (value - high.astype(F32)).astype(BF16)

    def cross_rhs(l, lanes):
        pieces = [nb_ref[:, lanes]]
        if l > 0:
            pieces = [jnp.zeros((32 * l, 256), BF16)] + pieces
        if l < 7:
            pieces = pieces + [jnp.zeros((32 * (7 - l), 256), BF16)]
        return jnp.concatenate(pieces, axis=0)

    def generate(accs):
        def step(t, carry):
            lanes = pl.ds(pl.multiple_of(t * 256, 256), 256)
            for l in range(8):
                used = [accs[l % 2][(l // 2 * 3 + g) % 4] for g in range(3)]
                pltpu.matmul_push_rhs(cross_rhs(l, lanes), staging_register=0, mxu_index=l % 2)
                for g in range(3):
                    pltpu.matmul_acc_lhs(
                        used[g], lhs_ref[g], load_staged_rhs=0 if g == 0 else None
                    )
                for g in range(3):
                    high, low = parts_of(jnp.exp2(pltpu.matmul_pop(used[g])))
                    kh_ref[g * 8 + l, t] = high
                    kl_ref[g * 8 + l, t] = low
            return carry

        return step

    def start_generation(*accs):
        for acc in accs:
            pltpu.matmul_pop(acc)
        for g in range(4):
            for k in range(2):
                chosen = sel_ref[g, k * 256 : min((k + 1) * 256, 384), :]
                if k == 1:
                    chosen = jnp.concatenate([chosen, jnp.zeros((128, 256), BF16)], axis=0)
                pltpu.matmul_push_rhs(chosen, staging_register=0, mxu_index=g % 2)
                pltpu.matmul_acc_lhs(accs[g], parts_ref[k], load_staged_rhs=0)
        for g in range(4):
            lhs_ref[g] = pltpu.matmul_pop(accs[g]).astype(BF16)

    def generate_range(first, last):
        def scoped(zero, one):
            for acc in (*zero, *one):
                pltpu.matmul_pop(acc)
            lax.fori_loop(first, last, generate((zero, one)), 0)

        pl.run_scoped(
            scoped,
            tuple(pltpu.ACC(0)((256, 256), F32) for _ in range(4)),
            tuple(pltpu.ACC(1)((256, 256), F32) for _ in range(4)),
        )

    for k, part in enumerate(split3(gp_ref[...])):
        parts_ref[k // 2, :, (k % 2) * 128 : (k % 2 + 1) * 128] = part
    parts_ref[1, :, 128:256] = jnp.zeros((DEVICES, 128), BF16)
    pl.run_scoped(start_generation, *[pltpu.ACC(g % 2)((256, 256), F32) for g in range(4)])

    generate_range(0, 2)

    for step in (1, 7, 2, 6):
        copies3[step - 1].wait_recv()
        forward(step)
    generate_range(2, 3)
    for step in (3, 5, 4):
        copies3[step - 1].wait_recv()
        forward(step)
    every3 = all_rows(g2_ref, NZ - 1, 4, 4)
    every4 = all_rows(g2_ref, NZ * len(plane), 5, 6)
    every5 = all_rows(g2_ref, NZ * NX * NY, 7, 8)

    def fifth_copy(k, dy, dx):
        rows = block_rows(lax.rem(y + NY - dy, NY), lax.rem(x + NX - dx, NX), core)
        return pltpu.make_async_remote_copy(
            src_ref=g2_ref.at[rows],
            dst_ref=g2_ref.at[rows],
            send_sem=sems.at[7],
            recv_sem=sems.at[8],
            device_id=partner,
            device_id_type=MESH,
        )

    copies5 = [fifth_copy(k, *d) for k, d in enumerate([(0, 0)] + plane)]
    copies5[0].start()
    every3.wait_send()
    generate_range(3, 7)
    every4.wait_recv()
    for copy in copies5[1:]:
        copy.start()
    every4.wait_send()
    generate_range(7, 8)
    turned = gp_ref[...].T
    scale_ref[...] = jnp.exp(
        -HALF_INV * (turned[32:64] ** 2 + turned[64:96] ** 2 + turned[96:128] ** 2)
    )
    every5.wait_recv()
    every5.wait_send()

    for j in range(8):
        block = g2_ref[:, j, :].T
        for q in range(4):
            l = 4 * j + q
            value = block[q * 32 : (q + 1) * 32] * scale_ref[l : l + 1, :]
            high = value.astype(BF16)
            wc_ref[l, 0:32, :] = high
            wc_ref[l, 32:64, :] = (value - high.astype(F32)).astype(BF16)

    def products(zero, one, high_accs, low_accs):
        accs = (zero, one)
        for acc in (*zero, *one, *high_accs, *low_accs):
            pltpu.matmul_pop(acc)

        def add(u, l, high, low):
            pltpu.matmul_push_rhs(high, staging_register=0, mxu_index=0)
            pltpu.matmul_acc_lhs(high_accs[u], wc_ref[l], load_staged_rhs=0)
            pltpu.matmul_push_rhs(low, staging_register=0, mxu_index=1)
            pltpu.matmul_acc_lhs(low_accs[u], wc_ref[l, 0:32], load_staged_rhs=0)

        def columns(i, carry):
            lanes = [pl.ds(pl.multiple_of((2 * i + u) * 256, 256), 256) for u in range(2)]

            def power(n):
                u, l = n // 8, n % 8
                pltpu.matmul_push_rhs(
                    cross_rhs(l, lanes[u]), staging_register=1, mxu_index=n % 2
                )
                pltpu.matmul_acc_lhs(accs[n % 2][(n // 2) % 2], lhs_ref[3], load_staged_rhs=1)

            power(0)
            power(1)
            for n in range(16):
                u, l = n // 8, n % 8
                t = 2 * i + u
                value = jnp.exp2(pltpu.matmul_pop(accs[n % 2][(n // 2) % 2]))
                if n < 14:
                    power(n + 2)
                for k in range(3 * l, 3 * l + 3):
                    add(u, k, kh_ref[k, t], kl_ref[k, t])
                add(u, 24 + l, *parts_of(value))
            for u in range(2):
                first = pltpu.matmul_pop(high_accs[u])
                total = first[0:32] + first[32:64] + pltpu.matmul_pop(low_accs[u])
                place_of = nodes_ref[:, lanes[u]]
                factor = jnp.exp(
                    -HALF_INV * jnp.sum(place_of * place_of, axis=0, keepdims=True)
                )
                base = jnp.concatenate([place_of] * 5 + [jnp.zeros((17, 256), F32)], axis=0)
                moved = total * factor + base
                tab_ref[:, lanes[u]] = moved
                for k, part in enumerate(split3(moved)):
                    t3_ref[k * 32 : (k + 1) * 32, lanes[u]] = part
            return carry

        lax.fori_loop(0, TILES // 2, columns, 0)

    pl.run_scoped(
        products,
        tuple(pltpu.ACC(0)((256, 256), F32) for _ in range(2)),
        tuple(pltpu.ACC(1)((256, 256), F32) for _ in range(2)),
        tuple(pltpu.ACC(0)((64, 256), F32) for _ in range(2)),
        tuple(pltpu.ACC(1)((32, 256), F32) for _ in range(2)),
    )

    def gather(accs, by_matmul, by_permute):
        for u, (p, q) in enumerate(by_matmul):
            index = jnp.concatenate([conn_ref[p : p + 1, :], conn_ref[q : q + 1, :]], axis=1)
            selected(accs, t3_ref, index.astype(F32), 16, u)
        for p in by_permute:
            for r, value in enumerate(permuted(tab_ref, conn_ref[p : p + 1, :], 16)):
                gat_ref[p * 32 + r * 8 : p * 32 + r * 8 + 8, :] = value
        for u, (p, q) in enumerate(by_matmul):
            parts = pltpu.matmul_pop(accs[u])
            value = parts[0:32] + parts[32:64] + parts[64:96]
            gat_ref[p * 32 : p * 32 + 32, :] = value[:, 0:128]
            gat_ref[q * 32 : q * 32 + 32, :] = value[:, 128:256]

    inside = [p for p in range(64) if p % 4 in (1, 2) and (p // 4) % 4 in (1, 2)]
    outside = [p for p in range(64) if p not in inside]

    def gather_stage(points, count):
        pairs = [(points[2 * u], points[2 * u + 1]) for u in range(count)]

        def scoped(*accs):
            for acc in accs:
                pltpu.matmul_pop(acc)
            gather(accs, pairs, points[2 * count :])

        pl.run_scoped(scoped, *[pltpu.ACC(u % 2)((96, 256), F32) for u in range(count)])

    gather_stage(outside, 16)

    derivative = lobatto_derivative()

    def rows(first, p):
        return gat_ref[pl.ds(p * 32 + first, 5, stride=3), :]

    def jacobian(p, directions):
        a, b, c = p // 16, (p // 4) % 4, p % 4
        lines = (
            (a, [k * 16 + b * 4 + c for k in range(4)]),
            (b, [a * 16 + k * 4 + c for k in range(4)]),
            (c, [a * 16 + b * 4 + k for k in range(4)]),
        )
        jac = [[None] * 3 for _ in range(3)]
        for i in range(3):
            for d in directions:
                at, points = lines[d]
                terms = [
                    float(derivative[at, k]) * rows(i, q)
                    for k, q in enumerate(points)
                    if derivative[at, k] != 0.0
                ]
                jac[i][d] = functools.reduce(jnp.add, terms)
        return jac

    def metric(jac, d, i):
        i1, i2, d1, d2 = (i + 1) % 3, (i + 2) % 3, (d + 1) % 3, (d + 2) % 3
        return jac[i1][d1] * jac[i2][d2] - jac[i1][d2] * jac[i2][d1]

    def normal(entries, speed):
        return entries[0] * speed[0] + entries[1] * speed[1] + entries[2] * speed[2]

    def face_flux(p, d):
        jac = jacobian(p, [k for k in range(3) if k != d])
        speed = [rows(15 + i, p) for i in range(3)]
        fl_ref[d - 1, p, 0:5, :] = normal([metric(jac, d, i) for i in range(3)], speed)

    def metrics(p):
        jac = jacobian(p, range(3))
        speed = [rows(15 + i, p) for i in range(3)]
        entries = [[metric(jac, d, i) for i in range(3)] for d in range(3)]
        det_ref[:, p, :] = (
            jac[0][0] * entries[0][0] + jac[0][1] * entries[1][0] + jac[0][2] * entries[2][0]
        )
        for d in range(3):
            flux_ref[:, d, p, :] = normal(entries[d], speed)

    fl_ref[...] = jnp.zeros_like(fl_ref)
    for p in range(64):
        if p % 4 in (0, 3):
            face_flux(p, 2)
        if (p // 4) % 4 in (0, 3):
            face_flux(p, 1)

    lane = lax.broadcasted_iota(jnp.int32, (8, 128), 1)

    def quarters(values):
        out = values[0]
        for q in range(1, 4):
            out = jnp.where(lane >= q * 32, values[q], out)
        return out

    for t in range(4):
        index = jnp.broadcast_to(
            jnp.concatenate([elem_ref[t : t + 1, :]] * 4, axis=1), (8, 128)
        )
        for a in range(4):
            if t < 2:
                points = [a * 16 + q * 4 + 3 * t for q in range(4)]
            else:
                points = [a * 16 + 12 * (t - 2) + q for q in range(4)]
            picked = quarters(
                [
                    jnp.take_along_axis(
                        fl_ref[1 - t // 2, p], index, axis=1, mode="promise_in_bounds"
                    )
                    for p in points
                ]
            )
            tr_ref[t, a] = picked if t % 2 else -picked

    across = [(0, beside[1], 1), (1, beside[0], 0), (2, beside[3], 3), (3, beside[2], 2)]
    copies6 = [
        pltpu.make_async_remote_copy(
            src_ref=tr_ref.at[t],
            dst_ref=rc_ref.at[slot],
            send_sem=sems.at[9],
            recv_sem=sems.at[10],
            device_id=device,
            device_id_type=MESH,
        )
        for t, device, slot in across
    ]
    for copy in copies6:
        copy.start()
    gather_stage(inside, 4)
    for p in range(64):
        metrics(p)
    stores = [
        pltpu.make_async_copy(det_ref, det_out, store.at[0]),
        pltpu.make_async_copy(flux_ref, flux_out, store.at[1]),
    ]
    for copy in stores:
        copy.start()
    every6 = pltpu.make_async_remote_copy(
        src_ref=tr_ref,
        dst_ref=rc_ref,
        send_sem=sems.at[9],
        recv_sem=sems.at[10],
        device_id=partner,
        device_id_type=MESH,
    )
    every6.wait_recv()
    every6.wait_send()

    for t in range(4):
        index = jnp.broadcast_to(
            jnp.concatenate([match_ref[t : t + 1, :] + 32 * q for q in range(4)], axis=1), (8, 128)
        )
        for a in range(4):
            own = tr_ref[t, a]
            other = jnp.take_along_axis(rc_ref[t, a], index, axis=1, mode="promise_in_bounds")
            if t == 0:
                other = jnp.where(jnp.broadcast_to(span == 0, (8, 128)), -own, other)
            if t == 1:
                other = jnp.where(
                    jnp.broadcast_to(span == NY * NCORE - 1, (8, 128)), -own, other
                )
            face_ref[t, a] = 0.5 * (own - other)
    for copy in stores:
        copy.wait()


def finish(
    det_in,
    flux_in,
    packed_in,
    det_out,
    flux_out,
    face_out,
    det_ref,
    flux_ref,
    packed_ref,
    face_ref,
    sem,
):
    pairs = ((det_in, det_ref, det_out), (flux_in, flux_ref, flux_out))
    packed = pltpu.make_async_copy(packed_in, packed_ref, sem.at[5])
    packed.start()
    loads = [pltpu.make_async_copy(a, b, sem.at[k]) for k, (a, b, _) in enumerate(pairs)]
    stores = [pltpu.make_async_copy(b, c, sem.at[k + 2]) for k, (_, b, c) in enumerate(pairs)]
    for copy in loads:
        copy.start()
    packed.wait()
    for t in range(4):
        for a in range(4):
            value = packed_ref[t, a]
            for q in range(4):
                face_ref[t, :, a * 4 + q, :] = value[0:5, q * 32 : (q + 1) * 32]
    for k in range(2):
        loads[k].wait()
        stores[k].start()
    stores.append(pltpu.make_async_copy(face_ref, face_out, sem.at[4]))
    stores[2].start()
    for copy in stores:
        copy.wait()


def on_device(
    node_pos, ctrl_pos, ctrl_ids, wing_shift, wing_speed, minv, conn, face_elem, face_match
):
    vmem = pl.BlockSpec(memory_space=pltpu.VMEM)
    hbm = pl.BlockSpec(memory_space=pltpu.HBM)
    dma = pltpu.SemaphoreType.DMA
    det, flux, packed = pl.pallas_call(
        kernel,
        out_shape=(
            jax.ShapeDtypeStruct((5, 64, 128), F32),
            jax.ShapeDtypeStruct((5, 3, 64, 128), F32),
            jax.ShapeDtypeStruct((4, 4, 8, 128), F32),
        ),
        in_specs=[hbm] * 10,
        out_specs=[hbm, hbm, vmem],
        scratch_shapes=[
            pltpu.VMEM((1, 32), jnp.int32),
            pltpu.VMEM((3, 32), F32),
            pltpu.VMEM((3, 2048), F32),
            pltpu.VMEM((15, 1024), F32),
            pltpu.VMEM((15, 1024), F32),
            pltpu.VMEM((32, 8192), F32),
            pltpu.VMEM((64, 128), jnp.int32),
            pltpu.VMEM((4, 32), jnp.int32),
            pltpu.VMEM((4, 32), jnp.int32),
            pltpu.VMEM((4, 384, 256), BF16),
            pltpu.VMEM((5, 64, 128), F32),
            pltpu.VMEM((5, 3, 64, 128), F32),
            pltpu.VMEM((1, 1, 128), F32),
            pltpu.VMEM((DEVICES, 1, 128), F32),
            pltpu.VMEM((DEVICES, 8, 128), F32),
            pltpu.VMEM((DEVICES, 128), F32),
            pltpu.VMEM((64, 128), F32),
            pltpu.VMEM((96, 1024), BF16),
            pltpu.VMEM((32, 1024), F32),
            pltpu.VMEM((96, 8192), BF16),
            pltpu.VMEM((96, 8192), BF16),
            pltpu.VMEM((96, 256), F32),
            pltpu.VMEM((32, 128), F32),
            pltpu.VMEM((32, DEVICES), F32),
            pltpu.VMEM((32, 64, DEVICES), BF16),
            pltpu.VMEM((STORED, TILES, 256, 256), BF16),
            pltpu.VMEM((STORED, TILES, 256, 256), BF16),
            pltpu.VMEM((2, DEVICES, 256), BF16),
            pltpu.VMEM((4, DEVICES, 256), BF16),
            pltpu.VMEM((32, 2048), BF16),
            pltpu.VMEM((96, 2048), BF16),
            pltpu.VMEM((32, 2048), F32),
            pltpu.VMEM((64 * 32, 128), F32),
            pltpu.VMEM((2, 64, 8, 128), F32),
            pltpu.VMEM((4, 4, 8, 128), F32),
            pltpu.VMEM((4, 4, 8, 128), F32),
            dma((11,)),
            dma((7,)),
            dma((10,)),
            dma((2,)),
        ],
        compiler_params=pltpu.CompilerParams(
            collective_id=0, has_side_effects=True, vmem_limit_bytes=67043328
        ),
        name="wing",
    )(
        ctrl_ids.reshape(1, 32),
        ctrl_pos,
        node_pos,
        wing_shift,
        wing_speed,
        minv,
        conn,
        face_elem.reshape(4, 32),
        face_match.reshape(4, 32),
        selection(),
    )
    det, flux, face = pl.pallas_call(
        finish,
        out_shape=(
            jax.ShapeDtypeStruct((5, 64, 128), F32),
            jax.ShapeDtypeStruct((5, 3, 64, 128), F32),
            jax.ShapeDtypeStruct((4, 5, 16, 32), F32),
        ),
        in_specs=[hbm] * 3,
        out_specs=[hbm] * 3,
        scratch_shapes=[
            pltpu.VMEM((5, 64, 128), F32),
            pltpu.VMEM((5, 3, 64, 128), F32),
            pltpu.VMEM((4, 4, 8, 128), F32),
            pltpu.VMEM((4, 5, 16, 32), F32),
            dma((6,)),
        ],
        name="wing_end",
    )(det, flux, packed)
    return det, flux, face.reshape(1, 1, 4, 5, 16, 32)


def solution(mesh):
    split = Mesh(mesh.devices.reshape(NY, NCORE, NZ, NX), SPAN_CHORD)
    return jax.shard_map(
        on_device,
        mesh=split,
        in_specs=(
            P(None, SPAN_CHORD),
            P(None, SPAN_CHORD),
            P(SPAN_CHORD),
            P(),
            P(),
            P(SPAN_CHORD, None),
            P(None, SPAN_CHORD),
            P(SPAN, CHORD, None, None),
            P(SPAN, CHORD, None, None),
        ),
        out_specs=(
            P(None, None, SPAN_CHORD),
            P(None, None, None, SPAN_CHORD),
            P(SPAN, CHORD, None, None, None, None),
        ),
        check_vma=False,
    )
```

```python
import functools

import jax
import jax.numpy as jnp
import numpy as np
from jax import lax
from jax.experimental import pallas as pl
from jax.experimental.pallas import tpu as pltpu
from jax.sharding import Mesh
from jax.sharding import PartitionSpec as P

SPAN_CHORD = ("y", "core", "z", "x")
SPAN = ("y", "core")
CHORD = ("z", "x")
NY, NCORE, NZ, NX = 4, 2, 8, 4
DEVICES = NY * NCORE * NZ * NX
GROUP = NCORE * NZ
MESH = pl.DeviceIdType.MESH
F32 = jnp.float32
BF16 = jnp.bfloat16

WIDTH = 0.1
HALF_INV = 1.0 / (2.0 * WIDTH**2)
CROSS = float(2.0 * HALF_INV * np.log2(np.e))
STORED = 24
TILES = 8
COLUMNS = 2
R_PERMUTED = 24
R_UNITS = (64 - R_PERMUTED) // 2


PAIRS = ((0, 0), (0, 1), (0, 2), (1, 0), (1, 1), (2, 0))


def selection():
    chosen = np.zeros((4, 384, 256), np.float32)
    for g in range(4):
        for l in range(8):
            for j, (part, _) in enumerate(PAIRS):
                for k in range(3):
                    chosen[g, part * 128 + 32 * (k + 1) + 8 * g + l, l * 32 + 3 * j + k] = 1.0
    return jnp.asarray(chosen, BF16)


def lobatto_derivative():
    points = np.array([-1.0, -1.0 / np.sqrt(5.0), 1.0 / np.sqrt(5.0), 1.0])
    barycentric = np.array(
        [
            1.0 / np.prod([points[t] - points[s] for s in range(4) if s != t])
            for t in range(4)
        ]
    )
    derivative = np.zeros((4, 4))
    for t in range(4):
        for s in range(4):
            if s != t:
                derivative[t, s] = barycentric[s] / barycentric[t] / (points[t] - points[s])
        derivative[t, t] = -np.sum(derivative[t])
    return derivative


def split3(value):
    high = value.astype(BF16)
    rest = value - high.astype(F32)
    middle = rest.astype(BF16)
    low = (rest - middle.astype(F32)).astype(BF16)
    return high, middle, low


def one_hot(index, blocks):
    width = index.shape[1]
    block = jnp.floor(index * (1.0 / 128.0))
    lane = (index - block * 128.0).astype(BF16)
    block = jnp.broadcast_to(block.astype(BF16), (128, width))
    row = lax.broadcasted_iota(jnp.int32, (128, width), 0).astype(F32).astype(BF16)
    one = jnp.ones((128, width), BF16)
    zero = jnp.zeros((128, width), BF16)
    inner = jnp.where(row == jnp.broadcast_to(lane, (128, width)), one, zero)
    return jnp.concatenate(
        [jnp.where(block == jnp.full((128, width), b, BF16), inner, zero) for b in range(blocks)],
        axis=0,
    )


def kernel(
    ids_in,
    ctrl_in,
    nodes_in,
    shift_in,
    speed_in,
    minv_in,
    conn_in,
    elem_in,
    match_in,
    sel_in,
    det_out,
    flux_out,
    face_ref,
    ids_ref,
    ctrl_ref,
    nodes_ref,
    shift_ref,
    speed_ref,
    minv_ref,
    conn_ref,
    elem_ref,
    match_ref,
    sel_ref,
    det_ref,
    flux_ref,
    own_ref,
    g1_ref,
    g2_ref,
    gp_ref,
    idr_ref,
    table_ref,
    plain_ref,
    r3_ref,
    m3_ref,
    cross_ref,
    wt_ref,
    scale_ref,
    wc_ref,
    kh_ref,
    kl_ref,
    parts_ref,
    lhs_ref,
    nb_ref,
    t3_ref,
    tab_ref,
    gat_ref,
    fl_ref,
    tr_ref,
    rc_ref,
    sems,
    recv3,
    load,
    store,
):
    y, core, z, x = (lax.axis_index(name) for name in SPAN_CHORD)
    group = y * NX + x
    place = core * NZ + z
    line = [(dc, dz) for dc in range(NCORE) for dz in range(NZ) if (dc, dz) != (0, 0)]
    plane = [(dy, dx) for dy in range(NY) for dx in range(NX) if (dy, dx) != (0, 0)]

    def line_device(dc, dz):
        return (y, lax.rem(core + dc, NCORE), lax.rem(z + dz, NZ), x)

    def plane_device(dy, dx):
        return (lax.rem(y + dy, NY), core, z, lax.rem(x + dx, NX))

    span = y * NCORE + core
    chord = z * NX + x

    def span_device(step):
        j = lax.rem(span + step + NY * NCORE, NY * NCORE)
        return (j // NCORE, lax.rem(j, NCORE), z, x)

    def chord_device(step):
        k = lax.rem(chord + step + NZ * NX, NZ * NX)
        return (y, core, k // NX, lax.rem(k, NX))

    partner = (y, 1 - core, z, x)
    beside = [span_device(1), span_device(-1), chord_device(1), chord_device(-1)]

    barrier = pltpu.get_barrier_semaphore()
    greeted = [line_device(*d) for d in line] + [plane_device(*d) for d in plane] + beside
    for device in greeted:
        pl.semaphore_signal(barrier, inc=1, device_id=device, device_id_type=MESH)

    loads = [
        pltpu.make_async_copy(source, target, load.at[k])
        for k, (source, target) in enumerate(
            (
                (ids_in, ids_ref),
                (ctrl_in, ctrl_ref),
                (shift_in, shift_ref),
                (speed_in, speed_ref),
                (minv_in, minv_ref),
                (nodes_in, nodes_ref),
                (conn_in, conn_ref),
                (elem_in, elem_ref),
                (match_in, match_ref),
                (sel_in, sel_ref),
            )
        )
    ]
    for copy in loads:
        copy.start()
    for copy in loads[:4]:
        copy.wait()
    own_ref[0] = jnp.concatenate(
        [ids_ref[...].astype(F32)] + [ctrl_ref[k : k + 1, :] for k in range(3)], axis=1
    )
    g1_ref[group * GROUP + place] = own_ref[0]
    table = jnp.concatenate(
        [shift_ref[...], speed_ref[...], jnp.zeros((2, shift_ref.shape[1]), F32)], axis=0
    )
    plain_ref[...] = table
    for k, part in enumerate(split3(table)):
        table_ref[k * 32 : (k + 1) * 32, :] = part

    pl.semaphore_wait(barrier, len(greeted))

    def first_copy(k, device):
        return pltpu.make_async_remote_copy(
            src_ref=own_ref,
            dst_ref=g1_ref.at[pl.ds(group * GROUP + place, 1)],
            send_sem=sems.at[0],
            recv_sem=sems.at[1],
            device_id=device,
            device_id_type=MESH,
        )

    copies1 = [first_copy(k, line_device(*d)) for k, d in enumerate(line)]
    for copy in copies1:
        copy.start()
    for copy in loads[4:]:
        copy.wait()
    for k, part in enumerate(split3(minv_ref[...])):
        m3_ref[k * 32 : (k + 1) * 32, :] = part
    node_parts = split3(nodes_ref[...] * CROSS)
    nb_ref[...] = jnp.concatenate(
        [node_parts[part].astype(F32) for _, part in PAIRS] + [jnp.zeros((14, 2048), F32)], axis=0
    ).astype(BF16)
    def all_rows(ref, count, sent, received):
        return pltpu.make_async_remote_copy(
            src_ref=ref.at[pl.ds(0, count)],
            dst_ref=ref.at[pl.ds(0, count)],
            send_sem=sems.at[sent],
            recv_sem=sems.at[received],
            device_id=partner,
            device_id_type=MESH,
        )

    every1 = all_rows(g1_ref, len(line), 0, 1)
    every2 = all_rows(g1_ref, len(plane) * GROUP, 2, 3)
    every1.wait_recv()

    def second_copy(k, device):
        rows = pl.ds(group * GROUP, GROUP)
        return pltpu.make_async_remote_copy(
            src_ref=g1_ref.at[rows],
            dst_ref=g1_ref.at[rows],
            send_sem=sems.at[2],
            recv_sem=sems.at[3],
            device_id=device,
            device_id_type=MESH,
        )

    copies2 = [second_copy(k, plane_device(*d)) for k, d in enumerate(plane)]
    for copy in copies2:
        copy.start()
    every1.wait_send()
    every2.wait_recv()
    every2.wait_send()

    gp_ref[...] = g1_ref[...].reshape(DEVICES, 128)
    for ny in range(NY):
        idr_ref[ny * GROUP : (ny + 1) * GROUP, :] = jnp.concatenate(
            [gp_ref[(ny * NX + q) * GROUP : (ny * NX + q + 1) * GROUP, 0:32] for q in range(NX)],
            axis=1,
        )

    def permuted(source_ref, index, blocks):
        node = jnp.broadcast_to(index, (8, 128))
        lane = node & 127
        block = node >> 7
        found = [None] * 4
        for k in range(blocks):
            here = block == k
            for r in range(4):
                taken = jnp.take_along_axis(
                    source_ref[r * 8 : r * 8 + 8, k * 128 : (k + 1) * 128],
                    lane,
                    axis=1,
                    mode="promise_in_bounds",
                )
                found[r] = taken if k == 0 else jnp.where(here, taken, found[r])
        return found

    def selected(accs, parts_ref, index, blocks, which):
        spread = one_hot(index, blocks)
        for k in range(blocks // 2):
            pltpu.matmul_push_rhs(
                spread[k * 256 : (k + 1) * 256], staging_register=0, mxu_index=which % 2
            )
            pltpu.matmul_acc_lhs(
                accs[which], parts_ref[:, k * 256 : (k + 1) * 256], load_staged_rhs=0
            )

    def first_stage(*accs):
        for acc in accs:
            pltpu.matmul_pop(acc)

        def right_side(i):
            for u in range(R_UNITS):
                pair = idr_ref[pl.ds((i * R_UNITS + u) * 2, 2), :]
                index = jnp.concatenate([pair[0:1], pair[1:2]], axis=1)
                selected(accs, table_ref, index, 8, u)
            for v in range(R_PERMUTED):
                row = 64 - R_PERMUTED + i * (R_PERMUTED) + v
                lanes = pl.ds(pl.multiple_of(row * 128, 128), 128)
                found = permuted(plain_ref, idr_ref[pl.ds(row, 1), :].astype(jnp.int32), 8)
                for k, part in enumerate(split3(jnp.concatenate(found, axis=0))):
                    r3_ref[k * 32 : (k + 1) * 32, lanes] = part
            for u in range(R_UNITS):
                lanes = pl.ds(pl.multiple_of((i * R_UNITS + u) * 256, 256), 256)
                r3_ref[:, lanes] = pltpu.matmul_pop(accs[u]).astype(BF16)

        right_side(0)

        for k in range(32):
            lanes = slice(k * 256, (k + 1) * 256)
            pltpu.matmul_push_rhs(
                jnp.concatenate([r3_ref[:, lanes], jnp.zeros((160, 256), BF16)], axis=0),
                staging_register=0,
                mxu_index=k % 2,
                transpose=True,
            )
            pltpu.matmul_acc_lhs(accs[k % 2], m3_ref[:, lanes], load_staged_rhs=0)
        cross_ref[...] = pltpu.matmul_pop(accs[0]) + pltpu.matmul_pop(accs[1])

    pl.run_scoped(first_stage, *[pltpu.ACC(u % 2)((96, 256), F32) for u in range(R_UNITS)])
    cross = cross_ref[...]

    def piece(a, b):
        return cross[a * 32 : (a + 1) * 32, b * 32 : (b + 1) * 32]

    weights = piece(0, 0) + (
        (piece(0, 1) + piece(1, 0)) + (piece(1, 1) + (piece(0, 2) + piece(2, 0)))
    )
    wt_ref[:, 0:32] = weights
    mine = group * GROUP + place
    g2_ref[mine] = jnp.concatenate(
        [wt_ref[pl.ds(q, 8, stride=4), 0:32] for q in range(4)], axis=1
    )

    def third_copy(k, device):
        return pltpu.make_async_remote_copy(
            src_ref=g2_ref.at[pl.ds(mine, 1)],
            dst_ref=g2_ref.at[pl.ds(mine, 1)],
            send_sem=sems.at[4],
            recv_sem=recv3.at[k],
            device_id=device,
            device_id_type=MESH,
        )

    copies3 = [third_copy(k, line_device(0, k + 1)) for k in range(NZ - 1)]
    for copy in copies3:
        copy.start()

    def block_rows(of_y, of_x, of_core):
        return pl.ds((of_y * NX + of_x) * GROUP + of_core * NZ, NZ)

    def fourth_copy(k, device, rows):
        return pltpu.make_async_remote_copy(
            src_ref=g2_ref.at[rows],
            dst_ref=g2_ref.at[rows],
            send_sem=sems.at[5],
            recv_sem=sems.at[6],
            device_id=device,
            device_id_type=MESH,
        )

    def forward(step):
        row = group * GROUP + core * NZ + lax.rem(z + NZ - step, NZ)
        for k, d in enumerate(plane):
            fourth_copy(k, plane_device(*d), pl.ds(row, 1)).start()

    forward(0)

    def parts_of(value):
        high = value.astype(BF16)
        return high, (value - high.astype(F32)).astype(BF16)

    def cross_rhs(l, lanes):
        pieces = [nb_ref[:, lanes]]
        if l > 0:
            pieces = [jnp.zeros((32 * l, 256), BF16)] + pieces
        if l < 7:
            pieces = pieces + [jnp.zeros((32 * (7 - l), 256), BF16)]
        return jnp.concatenate(pieces, axis=0)

    def generate(accs):
        def step(t, carry):
            lanes = pl.ds(pl.multiple_of(t * 256, 256), 256)
            for l in range(8):
                used = [accs[l % 2][(l // 2 * 3 + g) % 4] for g in range(3)]
                pltpu.matmul_push_rhs(cross_rhs(l, lanes), staging_register=0, mxu_index=l % 2)
                for g in range(3):
                    pltpu.matmul_acc_lhs(
                        used[g], lhs_ref[g], load_staged_rhs=0 if g == 0 else None
                    )
                for g in range(3):
                    high, low = parts_of(jnp.exp2(pltpu.matmul_pop(used[g])))
                    kh_ref[g * 8 + l, t] = high
                    kl_ref[g * 8 + l, t] = low
            return carry

        return step

    def start_generation(*accs):
        for acc in accs:
            pltpu.matmul_pop(acc)
        for g in range(4):
            for k in range(2):
                chosen = sel_ref[g, k * 256 : min((k + 1) * 256, 384), :]
                if k == 1:
                    chosen = jnp.concatenate([chosen, jnp.zeros((128, 256), BF16)], axis=0)
                pltpu.matmul_push_rhs(chosen, staging_register=0, mxu_index=g % 2)
                pltpu.matmul_acc_lhs(accs[g], parts_ref[k], load_staged_rhs=0)
        for g in range(4):
            lhs_ref[g] = pltpu.matmul_pop(accs[g]).astype(BF16)

    def generate_range(first, last):
        def scoped(zero, one):
            for acc in (*zero, *one):
                pltpu.matmul_pop(acc)
            lax.fori_loop(first, last, generate((zero, one)), 0)

        pl.run_scoped(
            scoped,
            tuple(pltpu.ACC(0)((256, 256), F32) for _ in range(4)),
            tuple(pltpu.ACC(1)((256, 256), F32) for _ in range(4)),
        )

    for k, part in enumerate(split3(gp_ref[...])):
        parts_ref[k // 2, :, (k % 2) * 128 : (k % 2 + 1) * 128] = part
    parts_ref[1, :, 128:256] = jnp.zeros((DEVICES, 128), BF16)
    pl.run_scoped(start_generation, *[pltpu.ACC(g % 2)((256, 256), F32) for g in range(4)])

    generate_range(0, 2)

    for step in (1, 7, 2, 6):
        copies3[step - 1].wait_recv()
        forward(step)
    generate_range(2, 3)
    for step in (3, 5, 4):
        copies3[step - 1].wait_recv()
        forward(step)
    every3 = all_rows(g2_ref, NZ - 1, 4, 4)
    every4 = all_rows(g2_ref, NZ * len(plane), 5, 6)
    every5 = all_rows(g2_ref, NZ * NX * NY, 7, 8)

    def fifth_copy(k, dy, dx):
        rows = block_rows(lax.rem(y + NY - dy, NY), lax.rem(x + NX - dx, NX), core)
        return pltpu.make_async_remote_copy(
            src_ref=g2_ref.at[rows],
            dst_ref=g2_ref.at[rows],
            send_sem=sems.at[7],
            recv_sem=sems.at[8],
            device_id=partner,
            device_id_type=MESH,
        )

    copies5 = [fifth_copy(k, *d) for k, d in enumerate([(0, 0)] + plane)]
    copies5[0].start()
    every3.wait_send()
    generate_range(3, 7)
    every4.wait_recv()
    for copy in copies5[1:]:
        copy.start()
    every4.wait_send()
    generate_range(7, 8)
    turned = gp_ref[...].T
    scale_ref[...] = jnp.exp(
        -HALF_INV * (turned[32:64] ** 2 + turned[64:96] ** 2 + turned[96:128] ** 2)
    )
    every5.wait_recv()
    every5.wait_send()

    for j in range(8):
        block = g2_ref[:, j, :].T
        for q in range(4):
            l = 4 * j + q
            value = block[q * 32 : (q + 1) * 32] * scale_ref[l : l + 1, :]
            high = value.astype(BF16)
            wc_ref[l, 0:32, :] = high
            wc_ref[l, 32:64, :] = (value - high.astype(F32)).astype(BF16)

    def products(zero, one, high_accs, low_accs):
        accs = (zero, one)
        for acc in (*zero, *one, *high_accs, *low_accs):
            pltpu.matmul_pop(acc)

        turn = [0, 0]

        def multiply(mxu, acc, lhs, rhs):
            register = turn[mxu] % 2
            turn[mxu] += 1
            pltpu.matmul_push_rhs(rhs, staging_register=register, mxu_index=mxu)
            pltpu.matmul_acc_lhs(acc, lhs, load_staged_rhs=register)

        def add(u, l, high, low):
            multiply(0, high_accs[u], wc_ref[l], high)
            multiply(1, low_accs[u], wc_ref[l, 0:32], low)

        def columns(i, carry):
            lanes = [
                pl.ds(pl.multiple_of((COLUMNS * i + u) * 256, 256), 256) for u in range(COLUMNS)
            ]

            def power(n):
                u, l = n // 8, n % 8
                multiply(n % 2, accs[n % 2][(n // 2) % 2], lhs_ref[3], cross_rhs(l, lanes[u]))

            power(0)
            power(1)
            def stored(n):
                u, l = n // 8, n % 8
                t = COLUMNS * i + u
                for k in range(3 * l, 3 * l + 3):
                    add(u, k, kh_ref[k, t], kl_ref[k, t])

            for n in range(8 * COLUMNS):
                u, l = n // 8, n % 8
                value = jnp.exp2(pltpu.matmul_pop(accs[n % 2][(n // 2) % 2]))
                if n < 8 * COLUMNS - 2:
                    power(n + 2)
                stored(n)
                add(u, 24 + l, *parts_of(value))
            for u in range(COLUMNS):
                first = pltpu.matmul_pop(high_accs[u])
                total = first[0:32] + first[32:64] + pltpu.matmul_pop(low_accs[u])
                place_of = nodes_ref[:, lanes[u]]
                factor = jnp.exp(
                    -HALF_INV * jnp.sum(place_of * place_of, axis=0, keepdims=True)
                )
                base = jnp.concatenate([place_of] * 5 + [jnp.zeros((17, 256), F32)], axis=0)
                moved = total * factor + base
                tab_ref[:, lanes[u]] = moved
                for k, part in enumerate(split3(moved)):
                    t3_ref[k * 32 : (k + 1) * 32, lanes[u]] = part
            return carry

        lax.fori_loop(0, TILES // COLUMNS, columns, 0)

    pl.run_scoped(
        products,
        tuple(pltpu.ACC(0)((256, 256), F32) for _ in range(2)),
        tuple(pltpu.ACC(1)((256, 256), F32) for _ in range(2)),
        tuple(pltpu.ACC(0)((64, 256), F32) for _ in range(COLUMNS)),
        tuple(pltpu.ACC(1)((32, 256), F32) for _ in range(COLUMNS)),
    )

    def gather(accs, by_matmul, by_permute):
        for u, (p, q) in enumerate(by_matmul):
            index = jnp.concatenate([conn_ref[p : p + 1, :], conn_ref[q : q + 1, :]], axis=1)
            selected(accs, t3_ref, index.astype(F32), 16, u)
        for p in by_permute:
            for r, value in enumerate(permuted(tab_ref, conn_ref[p : p + 1, :], 16)):
                gat_ref[p * 32 + r * 8 : p * 32 + r * 8 + 8, :] = value
        for u, (p, q) in enumerate(by_matmul):
            parts = pltpu.matmul_pop(accs[u])
            value = parts[0:32] + parts[32:64] + parts[64:96]
            gat_ref[p * 32 : p * 32 + 32, :] = value[:, 0:128]
            gat_ref[q * 32 : q * 32 + 32, :] = value[:, 128:256]

    chord_points = [p for p in range(64) if (p // 4) % 4 in (0, 3)]
    span_points = [p for p in range(64) if p not in chord_points and p % 4 in (0, 3)]
    inside = [p for p in range(64) if p not in chord_points + span_points]

    def gather_stage(points, count):
        pairs = [(points[2 * u], points[2 * u + 1]) for u in range(count)]

        def scoped(*accs):
            for acc in accs:
                pltpu.matmul_pop(acc)
            gather(accs, pairs, points[2 * count :])

        pl.run_scoped(scoped, *[pltpu.ACC(u % 2)((96, 256), F32) for u in range(count)])

    gather_stage(chord_points, 10)

    derivative = lobatto_derivative()

    def rows(first, p):
        return gat_ref[pl.ds(p * 32 + first, 5, stride=3), :]

    def jacobian(p, directions):
        a, b, c = p // 16, (p // 4) % 4, p % 4
        lines = (
            (a, [k * 16 + b * 4 + c for k in range(4)]),
            (b, [a * 16 + k * 4 + c for k in range(4)]),
            (c, [a * 16 + b * 4 + k for k in range(4)]),
        )
        jac = [[None] * 3 for _ in range(3)]
        for i in range(3):
            for d in directions:
                at, points = lines[d]
                terms = [
                    float(derivative[at, k]) * rows(i, q)
                    for k, q in enumerate(points)
                    if derivative[at, k] != 0.0
                ]
                jac[i][d] = functools.reduce(jnp.add, terms)
        return jac

    def metric(jac, d, i):
        i1, i2, d1, d2 = (i + 1) % 3, (i + 2) % 3, (d + 1) % 3, (d + 2) % 3
        return jac[i1][d1] * jac[i2][d2] - jac[i1][d2] * jac[i2][d1]

    def normal(entries, speed):
        return entries[0] * speed[0] + entries[1] * speed[1] + entries[2] * speed[2]

    def face_flux(p, d):
        jac = jacobian(p, [k for k in range(3) if k != d])
        speed = [rows(15 + i, p) for i in range(3)]
        fl_ref[d - 1, p, 0:5, :] = normal([metric(jac, d, i) for i in range(3)], speed)

    def metrics(p):
        jac = jacobian(p, range(3))
        speed = [rows(15 + i, p) for i in range(3)]
        entries = [[metric(jac, d, i) for i in range(3)] for d in range(3)]
        det_ref[:, p, :] = (
            jac[0][0] * entries[0][0] + jac[0][1] * entries[1][0] + jac[0][2] * entries[2][0]
        )
        for d in range(3):
            flux_ref[:, d, p, :] = normal(entries[d], speed)

    lane = lax.broadcasted_iota(jnp.int32, (8, 128), 1)

    def quarters(values):
        out = values[0]
        for q in range(1, 4):
            out = jnp.where(lane >= q * 32, values[q], out)
        return out

    across = {0: (beside[1], 1), 1: (beside[0], 0), 2: (beside[3], 3), 3: (beside[2], 2)}

    def trace(t):
        index = jnp.broadcast_to(
            jnp.concatenate([elem_ref[t : t + 1, :]] * 4, axis=1), (8, 128)
        )
        for a in range(4):
            if t < 2:
                points = [a * 16 + q * 4 + 3 * t for q in range(4)]
            else:
                points = [a * 16 + 12 * (t - 2) + q for q in range(4)]
            picked = quarters(
                [
                    jnp.take_along_axis(
                        fl_ref[1 - t // 2, p], index, axis=1, mode="promise_in_bounds"
                    )
                    for p in points
                ]
            )
            tr_ref[t, a] = picked if t % 2 else -picked

    def send(t):
        device, slot = across[t]
        pltpu.make_async_remote_copy(
            src_ref=tr_ref.at[t],
            dst_ref=rc_ref.at[slot],
            send_sem=sems.at[9],
            recv_sem=sems.at[10],
            device_id=device,
            device_id_type=MESH,
        ).start()

    fl_ref[...] = jnp.zeros_like(fl_ref)
    for p in chord_points:
        face_flux(p, 1)
    for t in (2, 3):
        trace(t)
    for t in (2, 3):
        send(t)
    gather_stage(span_points, 4)
    for p in range(64):
        if p % 4 in (0, 3):
            face_flux(p, 2)
    for t in (0, 1):
        trace(t)
    for t in (0, 1):
        send(t)
    gather_stage(inside, 4)
    for p in range(64):
        metrics(p)
    stores = [
        pltpu.make_async_copy(det_ref, det_out, store.at[0]),
        pltpu.make_async_copy(flux_ref, flux_out, store.at[1]),
    ]
    for copy in stores:
        copy.start()
    every6 = pltpu.make_async_remote_copy(
        src_ref=tr_ref,
        dst_ref=rc_ref,
        send_sem=sems.at[9],
        recv_sem=sems.at[10],
        device_id=partner,
        device_id_type=MESH,
    )
    every6.wait_recv()
    every6.wait_send()

    for t in range(4):
        index = jnp.broadcast_to(
            jnp.concatenate([match_ref[t : t + 1, :] + 32 * q for q in range(4)], axis=1), (8, 128)
        )
        for a in range(4):
            own = tr_ref[t, a]
            other = jnp.take_along_axis(rc_ref[t, a], index, axis=1, mode="promise_in_bounds")
            if t == 0:
                other = jnp.where(jnp.broadcast_to(span == 0, (8, 128)), -own, other)
            if t == 1:
                other = jnp.where(
                    jnp.broadcast_to(span == NY * NCORE - 1, (8, 128)), -own, other
                )
            face_ref[t, a] = 0.5 * (own - other)
    for copy in stores:
        copy.wait()


def finish(
    det_in,
    flux_in,
    packed_in,
    det_out,
    flux_out,
    face_out,
    det_ref,
    flux_ref,
    packed_ref,
    face_ref,
    sem,
):
    pairs = ((det_in, det_ref, det_out), (flux_in, flux_ref, flux_out))
    packed = pltpu.make_async_copy(packed_in, packed_ref, sem.at[5])
    packed.start()
    loads = [pltpu.make_async_copy(a, b, sem.at[k]) for k, (a, b, _) in enumerate(pairs)]
    stores = [pltpu.make_async_copy(b, c, sem.at[k + 2]) for k, (_, b, c) in enumerate(pairs)]
    for copy in loads:
        copy.start()
    packed.wait()
    for t in range(4):
        for a in range(4):
            value = packed_ref[t, a]
            for q in range(4):
                face_ref[t, :, a * 4 + q, :] = value[0:5, q * 32 : (q + 1) * 32]
    for k in range(2):
        loads[k].wait()
        stores[k].start()
    stores.append(pltpu.make_async_copy(face_ref, face_out, sem.at[4]))
    stores[2].start()
    for copy in stores:
        copy.wait()


def on_device(
    node_pos, ctrl_pos, ctrl_ids, wing_shift, wing_speed, minv, conn, face_elem, face_match
):
    vmem = pl.BlockSpec(memory_space=pltpu.VMEM)
    hbm = pl.BlockSpec(memory_space=pltpu.HBM)
    dma = pltpu.SemaphoreType.DMA
    det, flux, packed = pl.pallas_call(
        kernel,
        out_shape=(
            jax.ShapeDtypeStruct((5, 64, 128), F32),
            jax.ShapeDtypeStruct((5, 3, 64, 128), F32),
            jax.ShapeDtypeStruct((4, 4, 8, 128), F32),
        ),
        in_specs=[hbm] * 10,
        out_specs=[hbm, hbm, vmem],
        scratch_shapes=[
            pltpu.VMEM((1, 32), jnp.int32),
            pltpu.VMEM((3, 32), F32),
            pltpu.VMEM((3, 2048), F32),
            pltpu.VMEM((15, 1024), F32),
            pltpu.VMEM((15, 1024), F32),
            pltpu.VMEM((32, 8192), F32),
            pltpu.VMEM((64, 128), jnp.int32),
            pltpu.VMEM((4, 32), jnp.int32),
            pltpu.VMEM((4, 32), jnp.int32),
            pltpu.VMEM((4, 384, 256), BF16),
            pltpu.VMEM((5, 64, 128), F32),
            pltpu.VMEM((5, 3, 64, 128), F32),
            pltpu.VMEM((1, 1, 128), F32),
            pltpu.VMEM((DEVICES, 1, 128), F32),
            pltpu.VMEM((DEVICES, 8, 128), F32),
            pltpu.VMEM((DEVICES, 128), F32),
            pltpu.VMEM((64, 128), F32),
            pltpu.VMEM((96, 1024), BF16),
            pltpu.VMEM((32, 1024), F32),
            pltpu.VMEM((96, 8192), BF16),
            pltpu.VMEM((96, 8192), BF16),
            pltpu.VMEM((96, 256), F32),
            pltpu.VMEM((32, 128), F32),
            pltpu.VMEM((32, DEVICES), F32),
            pltpu.VMEM((32, 64, DEVICES), BF16),
            pltpu.VMEM((STORED, TILES, 256, 256), BF16),
            pltpu.VMEM((STORED, TILES, 256, 256), BF16),
            pltpu.VMEM((2, DEVICES, 256), BF16),
            pltpu.VMEM((4, DEVICES, 256), BF16),
            pltpu.VMEM((32, 2048), BF16),
            pltpu.VMEM((96, 2048), BF16),
            pltpu.VMEM((32, 2048), F32),
            pltpu.VMEM((64 * 32, 128), F32),
            pltpu.VMEM((2, 64, 8, 128), F32),
            pltpu.VMEM((4, 4, 8, 128), F32),
            pltpu.VMEM((4, 4, 8, 128), F32),
            dma((11,)),
            dma((7,)),
            dma((10,)),
            dma((2,)),
        ],
        compiler_params=pltpu.CompilerParams(
            collective_id=0, has_side_effects=True, vmem_limit_bytes=67043328
        ),
        name="wing",
    )(
        ctrl_ids.reshape(1, 32),
        ctrl_pos,
        node_pos,
        wing_shift,
        wing_speed,
        minv,
        conn,
        face_elem.reshape(4, 32),
        face_match.reshape(4, 32),
        selection(),
    )
    det, flux, face = pl.pallas_call(
        finish,
        out_shape=(
            jax.ShapeDtypeStruct((5, 64, 128), F32),
            jax.ShapeDtypeStruct((5, 3, 64, 128), F32),
            jax.ShapeDtypeStruct((4, 5, 16, 32), F32),
        ),
        in_specs=[hbm] * 3,
        out_specs=[hbm] * 3,
        scratch_shapes=[
            pltpu.VMEM((5, 64, 128), F32),
            pltpu.VMEM((5, 3, 64, 128), F32),
            pltpu.VMEM((4, 4, 8, 128), F32),
            pltpu.VMEM((4, 5, 16, 32), F32),
            dma((6,)),
        ],
        name="wing_end",
    )(det, flux, packed)
    return det, flux, face.reshape(1, 1, 4, 5, 16, 32)


def solution(mesh):
    split = Mesh(mesh.devices.reshape(NY, NCORE, NZ, NX), SPAN_CHORD)
    return jax.shard_map(
        on_device,
        mesh=split,
        in_specs=(
            P(None, SPAN_CHORD),
            P(None, SPAN_CHORD),
            P(SPAN_CHORD),
            P(),
            P(),
            P(SPAN_CHORD, None),
            P(None, SPAN_CHORD),
            P(SPAN, CHORD, None, None),
            P(SPAN, CHORD, None, None),
        ),
        out_specs=(
            P(None, None, SPAN_CHORD),
            P(None, None, None, SPAN_CHORD),
            P(SPAN, CHORD, None, None, None, None),
        ),
        check_vma=False,
    )
```

```python
import functools

import jax
import jax.numpy as jnp
import numpy as np
from jax import lax
from jax.experimental import pallas as pl
from jax.experimental.pallas import tpu as pltpu
from jax.sharding import Mesh
from jax.sharding import PartitionSpec as P

SPAN_CHORD = ("y", "core", "z", "x")
SPAN = ("y", "core")
CHORD = ("z", "x")
NY, NCORE, NZ, NX = 4, 2, 8, 4
DEVICES = NY * NCORE * NZ * NX
GROUP = NCORE * NZ
MESH = pl.DeviceIdType.MESH
F32 = jnp.float32
BF16 = jnp.bfloat16

WIDTH = 0.1
HALF_INV = 1.0 / (2.0 * WIDTH**2)
CROSS = float(2.0 * HALF_INV * np.log2(np.e))
STORED = 24
TILES = 8
COLUMNS = 2
R_PERMUTED = 32
R_UNITS = (64 - R_PERMUTED) // 2


PAIRS = ((0, 0), (0, 1), (0, 2), (1, 0), (1, 1), (2, 0))


def selection():
    chosen = np.zeros((4, 384, 256), np.float32)
    for g in range(4):
        for l in range(8):
            for j, (part, _) in enumerate(PAIRS):
                for k in range(3):
                    chosen[g, part * 128 + 32 * (k + 1) + 8 * g + l, l * 32 + 3 * j + k] = 1.0
    return jnp.asarray(chosen, BF16)


def lobatto_derivative():
    points = np.array([-1.0, -1.0 / np.sqrt(5.0), 1.0 / np.sqrt(5.0), 1.0])
    barycentric = np.array(
        [
            1.0 / np.prod([points[t] - points[s] for s in range(4) if s != t])
            for t in range(4)
        ]
    )
    derivative = np.zeros((4, 4))
    for t in range(4):
        for s in range(4):
            if s != t:
                derivative[t, s] = barycentric[s] / barycentric[t] / (points[t] - points[s])
        derivative[t, t] = -np.sum(derivative[t])
    return derivative


def split3(value):
    high = value.astype(BF16)
    rest = value - high.astype(F32)
    middle = rest.astype(BF16)
    low = (rest - middle.astype(F32)).astype(BF16)
    return high, middle, low


def one_hot(index, blocks):
    width = index.shape[1]
    block = jnp.floor(index * (1.0 / 128.0))
    lane = (index - block * 128.0).astype(BF16)
    block = jnp.broadcast_to(block.astype(BF16), (128, width))
    row = lax.broadcasted_iota(jnp.int32, (128, width), 0).astype(F32).astype(BF16)
    one = jnp.ones((128, width), BF16)
    zero = jnp.zeros((128, width), BF16)
    inner = jnp.where(row == jnp.broadcast_to(lane, (128, width)), one, zero)
    return jnp.concatenate(
        [jnp.where(block == jnp.full((128, width), b, BF16), inner, zero) for b in range(blocks)],
        axis=0,
    )


def kernel(
    ids_in,
    ctrl_in,
    nodes_in,
    shift_in,
    speed_in,
    minv_in,
    conn_in,
    elem_in,
    match_in,
    sel_in,
    det_out,
    flux_out,
    face_ref,
    ids_ref,
    ctrl_ref,
    nodes_ref,
    shift_ref,
    speed_ref,
    minv_ref,
    conn_ref,
    elem_ref,
    match_ref,
    sel_ref,
    det_ref,
    flux_ref,
    own_ref,
    g1_ref,
    g2_ref,
    gp_ref,
    idr_ref,
    table_ref,
    plain_ref,
    r3_ref,
    m3_ref,
    cross_ref,
    wt_ref,
    scale_ref,
    wc_ref,
    kh_ref,
    kl_ref,
    parts_ref,
    lhs_ref,
    nb_ref,
    t3_ref,
    tab_ref,
    gat_ref,
    fl_ref,
    tr_ref,
    rc_ref,
    sems,
    recv3,
    load,
    store,
):
    y, core, z, x = (lax.axis_index(name) for name in SPAN_CHORD)
    group = y * NX + x
    place = core * NZ + z
    line = [(dc, dz) for dc in range(NCORE) for dz in range(NZ) if (dc, dz) != (0, 0)]
    plane = [(dy, dx) for dy in range(NY) for dx in range(NX) if (dy, dx) != (0, 0)]

    near = [dy != 2 and dx != 2 for dy, dx in plane]

    def line_device(dc, dz):
        return (y, lax.rem(core + dc, NCORE), lax.rem(z + dz, NZ), x)

    def plane_device(dy, dx):
        return (lax.rem(y + dy, NY), core, z, lax.rem(x + dx, NX))

    span = y * NCORE + core
    chord = z * NX + x

    def span_device(step):
        j = lax.rem(span + step + NY * NCORE, NY * NCORE)
        return (j // NCORE, lax.rem(j, NCORE), z, x)

    def chord_device(step):
        k = lax.rem(chord + step + NZ * NX, NZ * NX)
        return (y, core, k // NX, lax.rem(k, NX))

    partner = (y, 1 - core, z, x)
    beside = [span_device(1), span_device(-1), chord_device(1), chord_device(-1)]

    barrier = pltpu.get_barrier_semaphore()
    greeted = [line_device(*d) for d in line] + [plane_device(*d) for d in plane] + beside
    for device in greeted:
        pl.semaphore_signal(barrier, inc=1, device_id=device, device_id_type=MESH)

    loads = [
        pltpu.make_async_copy(source, target, load.at[k])
        for k, (source, target) in enumerate(
            (
                (ids_in, ids_ref),
                (ctrl_in, ctrl_ref),
                (shift_in, shift_ref),
                (speed_in, speed_ref),
                (minv_in, minv_ref),
                (nodes_in, nodes_ref),
                (conn_in, conn_ref),
                (elem_in, elem_ref),
                (match_in, match_ref),
                (sel_in, sel_ref),
            )
        )
    ]
    for copy in loads:
        copy.start()
    for copy in loads[:2]:
        copy.wait()
    own_ref[0] = jnp.concatenate(
        [ids_ref[...].astype(F32)] + [ctrl_ref[k : k + 1, :] for k in range(3)], axis=1
    )
    g1_ref[group * GROUP + place] = own_ref[0]
    pl.semaphore_wait(barrier, len(greeted))

    def first_copy(k, device):
        return pltpu.make_async_remote_copy(
            src_ref=own_ref,
            dst_ref=g1_ref.at[pl.ds(group * GROUP + place, 1)],
            send_sem=sems.at[0],
            recv_sem=sems.at[1],
            device_id=device,
            device_id_type=MESH,
        )

    copies1 = [first_copy(k, line_device(*d)) for k, d in enumerate(line)]
    for copy in copies1:
        copy.start()
    for copy in loads[2:]:
        copy.wait()
    table = jnp.concatenate(
        [shift_ref[...], speed_ref[...], jnp.zeros((2, shift_ref.shape[1]), F32)], axis=0
    )
    plain_ref[...] = table
    for k, part in enumerate(split3(table)):
        table_ref[k * 32 : (k + 1) * 32, :] = part
    for k, part in enumerate(split3(minv_ref[...])):
        m3_ref[k * 32 : (k + 1) * 32, :] = part
    node_parts = split3(nodes_ref[...] * CROSS)
    nb_ref[...] = jnp.concatenate(
        [node_parts[part].astype(F32) for _, part in PAIRS] + [jnp.zeros((14, 2048), F32)], axis=0
    ).astype(BF16)
    def all_rows(ref, count, sent, received):
        return pltpu.make_async_remote_copy(
            src_ref=ref.at[pl.ds(0, count)],
            dst_ref=ref.at[pl.ds(0, count)],
            send_sem=sems.at[sent],
            recv_sem=sems.at[received],
            device_id=partner,
            device_id_type=MESH,
        )

    every1 = all_rows(g1_ref, len(line), 0, 1)
    every2 = all_rows(g1_ref, len(plane) * GROUP, 2, 3)
    every1.wait_recv()

    def second_copy(k, device):
        rows = pl.ds(group * GROUP, GROUP)
        return pltpu.make_async_remote_copy(
            src_ref=g1_ref.at[rows],
            dst_ref=g1_ref.at[rows],
            send_sem=sems.at[2],
            recv_sem=sems.at[3],
            device_id=device,
            device_id_type=MESH,
        )

    copies2 = [second_copy(k, plane_device(*d)) for k, d in enumerate(plane)]
    for copy in copies2:
        copy.start()
    every1.wait_send()
    every2.wait_recv()
    every2.wait_send()

    gp_ref[...] = g1_ref[...].reshape(DEVICES, 128)
    for ny in range(NY):
        idr_ref[ny * GROUP : (ny + 1) * GROUP, :] = jnp.concatenate(
            [gp_ref[(ny * NX + q) * GROUP : (ny * NX + q + 1) * GROUP, 0:32] for q in range(NX)],
            axis=1,
        )

    def permuted(source_ref, index, blocks):
        node = jnp.broadcast_to(index, (8, 128))
        lane = node & 127
        block = node >> 7
        found = [None] * 4
        for k in range(blocks):
            here = block == k
            for r in range(4):
                taken = jnp.take_along_axis(
                    source_ref[r * 8 : r * 8 + 8, k * 128 : (k + 1) * 128],
                    lane,
                    axis=1,
                    mode="promise_in_bounds",
                )
                found[r] = taken if k == 0 else jnp.where(here, taken, found[r])
        return found

    def selected(accs, parts_ref, index, blocks, which):
        spread = one_hot(index, blocks)
        for k in range(blocks // 2):
            pltpu.matmul_push_rhs(
                spread[k * 256 : (k + 1) * 256], staging_register=0, mxu_index=which % 2
            )
            pltpu.matmul_acc_lhs(
                accs[which], parts_ref[:, k * 256 : (k + 1) * 256], load_staged_rhs=0
            )

    def first_stage(*accs):
        for acc in accs:
            pltpu.matmul_pop(acc)

        def right_side(i):
            for u in range(R_UNITS):
                pair = idr_ref[pl.ds((i * R_UNITS + u) * 2, 2), :]
                index = jnp.concatenate([pair[0:1], pair[1:2]], axis=1)
                selected(accs, table_ref, index, 8, u)
            for v in range(R_PERMUTED):
                row = 64 - R_PERMUTED + i * (R_PERMUTED) + v
                lanes = pl.ds(pl.multiple_of(row * 128, 128), 128)
                found = permuted(plain_ref, idr_ref[pl.ds(row, 1), :].astype(jnp.int32), 8)
                for k, part in enumerate(split3(jnp.concatenate(found, axis=0))):
                    r3_ref[k * 32 : (k + 1) * 32, lanes] = part
            for u in range(R_UNITS):
                lanes = pl.ds(pl.multiple_of((i * R_UNITS + u) * 256, 256), 256)
                r3_ref[:, lanes] = pltpu.matmul_pop(accs[u]).astype(BF16)

        right_side(0)

        for k in range(32):
            lanes = slice(k * 256, (k + 1) * 256)
            pltpu.matmul_push_rhs(
                jnp.concatenate([r3_ref[:, lanes], jnp.zeros((160, 256), BF16)], axis=0),
                staging_register=0,
                mxu_index=k % 2,
                transpose=True,
            )
            pltpu.matmul_acc_lhs(accs[k % 2], m3_ref[:, lanes], load_staged_rhs=0)
        cross_ref[...] = pltpu.matmul_pop(accs[0]) + pltpu.matmul_pop(accs[1])

    pl.run_scoped(first_stage, *[pltpu.ACC(u % 2)((96, 256), F32) for u in range(R_UNITS)])
    cross = cross_ref[...]

    def piece(a, b):
        return cross[a * 32 : (a + 1) * 32, b * 32 : (b + 1) * 32]

    weights = piece(0, 0) + (
        (piece(0, 1) + piece(1, 0)) + (piece(1, 1) + (piece(0, 2) + piece(2, 0)))
    )
    wt_ref[:, 0:32] = weights
    mine = group * GROUP + place
    g2_ref[mine] = jnp.concatenate(
        [wt_ref[pl.ds(q, 8, stride=4), 0:32] for q in range(4)], axis=1
    )

    def third_copy(k, device):
        return pltpu.make_async_remote_copy(
            src_ref=g2_ref.at[pl.ds(mine, 1)],
            dst_ref=g2_ref.at[pl.ds(mine, 1)],
            send_sem=sems.at[4],
            recv_sem=recv3.at[k],
            device_id=device,
            device_id_type=MESH,
        )

    copies3 = [third_copy(k, line_device(0, k + 1)) for k in range(NZ - 1)]
    for copy in copies3:
        copy.start()

    def block_rows(of_y, of_x, of_core):
        return pl.ds((of_y * NX + of_x) * GROUP + of_core * NZ, NZ)

    def fourth_copy(k, device, rows):
        return pltpu.make_async_remote_copy(
            src_ref=g2_ref.at[rows],
            dst_ref=g2_ref.at[rows],
            send_sem=sems.at[5],
            recv_sem=sems.at[6 if near[k] else 11],
            device_id=device,
            device_id_type=MESH,
        )

    def forward(step):
        row = group * GROUP + core * NZ + lax.rem(z + NZ - step, NZ)
        for k, d in enumerate(plane):
            fourth_copy(k, plane_device(*d), pl.ds(row, 1)).start()

    forward(0)

    def parts_of(value):
        high = value.astype(BF16)
        return high, (value - high.astype(F32)).astype(BF16)

    def cross_rhs(l, lanes):
        pieces = [nb_ref[:, lanes]]
        if l > 0:
            pieces = [jnp.zeros((32 * l, 256), BF16)] + pieces
        if l < 7:
            pieces = pieces + [jnp.zeros((32 * (7 - l), 256), BF16)]
        return jnp.concatenate(pieces, axis=0)

    def generate(accs):
        def step(t, carry):
            lanes = pl.ds(pl.multiple_of(t * 256, 256), 256)
            for l in range(8):
                used = [accs[l % 2][(l // 2 * 3 + g) % 4] for g in range(3)]
                pltpu.matmul_push_rhs(cross_rhs(l, lanes), staging_register=0, mxu_index=l % 2)
                for g in range(3):
                    pltpu.matmul_acc_lhs(
                        used[g], lhs_ref[g], load_staged_rhs=0 if g == 0 else None
                    )
                for g in range(3):
                    high, low = parts_of(jnp.exp2(pltpu.matmul_pop(used[g])))
                    kh_ref[g * 8 + l, t] = high
                    kl_ref[g * 8 + l, t] = low
            return carry

        return step

    def start_generation(*accs):
        for acc in accs:
            pltpu.matmul_pop(acc)
        for g in range(4):
            for k in range(2):
                chosen = sel_ref[g, k * 256 : min((k + 1) * 256, 384), :]
                if k == 1:
                    chosen = jnp.concatenate([chosen, jnp.zeros((128, 256), BF16)], axis=0)
                pltpu.matmul_push_rhs(chosen, staging_register=0, mxu_index=g % 2)
                pltpu.matmul_acc_lhs(accs[g], parts_ref[k], load_staged_rhs=0)
        for g in range(4):
            lhs_ref[g] = pltpu.matmul_pop(accs[g]).astype(BF16)

    def generate_range(first, last):
        def scoped(zero, one):
            for acc in (*zero, *one):
                pltpu.matmul_pop(acc)
            lax.fori_loop(first, last, generate((zero, one)), 0)

        pl.run_scoped(
            scoped,
            tuple(pltpu.ACC(0)((256, 256), F32) for _ in range(4)),
            tuple(pltpu.ACC(1)((256, 256), F32) for _ in range(4)),
        )

    for k, part in enumerate(split3(gp_ref[...])):
        parts_ref[k // 2, :, (k % 2) * 128 : (k % 2 + 1) * 128] = part
    parts_ref[1, :, 128:256] = jnp.zeros((DEVICES, 128), BF16)
    pl.run_scoped(start_generation, *[pltpu.ACC(g % 2)((256, 256), F32) for g in range(4)])

    generate_range(0, 2)

    for step in (1, 7, 2, 6):
        copies3[step - 1].wait_recv()
        forward(step)
    generate_range(2, 3)
    for step in (3, 5, 4):
        copies3[step - 1].wait_recv()
        forward(step)
    every3 = all_rows(g2_ref, NZ - 1, 4, 4)
    every4 = all_rows(g2_ref, NZ * len(plane), 5, 6)
    every5 = all_rows(g2_ref, NZ * NX * NY, 7, 8)

    def fifth_copy(k, dy, dx):
        rows = block_rows(lax.rem(y + NY - dy, NY), lax.rem(x + NX - dx, NX), core)
        return pltpu.make_async_remote_copy(
            src_ref=g2_ref.at[rows],
            dst_ref=g2_ref.at[rows],
            send_sem=sems.at[7],
            recv_sem=sems.at[8],
            device_id=partner,
            device_id_type=MESH,
        )

    copies5 = [fifth_copy(k, *d) for k, d in enumerate([(0, 0)] + plane)]
    copies5[0].start()
    every3.wait_send()
    generate_range(3, 6)
    all_rows(g2_ref, NZ * sum(near), 5, 6).wait_recv()
    for copy, close in zip(copies5[1:], near):
        if close:
            copy.start()
    generate_range(6, 7)
    all_rows(g2_ref, NZ * (len(near) - sum(near)), 5, 11).wait_recv()
    for copy, close in zip(copies5[1:], near):
        if not close:
            copy.start()
    every4.wait_send()
    generate_range(7, 8)
    turned = gp_ref[...].T
    scale_ref[...] = jnp.exp(
        -HALF_INV * (turned[32:64] ** 2 + turned[64:96] ** 2 + turned[96:128] ** 2)
    )
    every5.wait_recv()
    every5.wait_send()

    for j in range(8):
        block = g2_ref[:, j, :].T
        for q in range(4):
            l = 4 * j + q
            value = block[q * 32 : (q + 1) * 32] * scale_ref[l : l + 1, :]
            high = value.astype(BF16)
            wc_ref[l, 0:32, :] = high
            wc_ref[l, 32:64, :] = (value - high.astype(F32)).astype(BF16)

    def products(zero, one, high_accs, low_accs):
        accs = (zero, one)
        for acc in (*zero, *one, *high_accs, *low_accs):
            pltpu.matmul_pop(acc)

        turn = [0, 0]

        def multiply(mxu, acc, lhs, rhs):
            register = turn[mxu] % 2
            turn[mxu] += 1
            pltpu.matmul_push_rhs(rhs, staging_register=register, mxu_index=mxu)
            pltpu.matmul_acc_lhs(acc, lhs, load_staged_rhs=register)

        def add(u, l, high, low):
            multiply(0, high_accs[u], wc_ref[l], high)
            multiply(1, low_accs[u], wc_ref[l, 0:32], low)

        def columns(i, carry):
            lanes = [
                pl.ds(pl.multiple_of((COLUMNS * i + u) * 256, 256), 256) for u in range(COLUMNS)
            ]

            def power(n):
                u, l = n // 8, n % 8
                multiply(n % 2, accs[n % 2][(n // 2) % 2], lhs_ref[3], cross_rhs(l, lanes[u]))

            power(0)
            power(1)
            def stored(n):
                u, l = n // 8, n % 8
                t = COLUMNS * i + u
                for k in range(3 * l, 3 * l + 3):
                    add(u, k, kh_ref[k, t], kl_ref[k, t])

            for n in range(8 * COLUMNS):
                u, l = n // 8, n % 8
                value = jnp.exp2(pltpu.matmul_pop(accs[n % 2][(n // 2) % 2]))
                if n < 8 * COLUMNS - 2:
                    power(n + 2)
                stored(n)
                add(u, 24 + l, *parts_of(value))
            for u in range(COLUMNS):
                first = pltpu.matmul_pop(high_accs[u])
                total = first[0:32] + first[32:64] + pltpu.matmul_pop(low_accs[u])
                place_of = nodes_ref[:, lanes[u]]
                factor = jnp.exp(
                    -HALF_INV * jnp.sum(place_of * place_of, axis=0, keepdims=True)
                )
                base = jnp.concatenate([place_of] * 5 + [jnp.zeros((17, 256), F32)], axis=0)
                moved = total * factor + base
                tab_ref[:, lanes[u]] = moved
                for k, part in enumerate(split3(moved)):
                    t3_ref[k * 32 : (k + 1) * 32, lanes[u]] = part
            return carry

        lax.fori_loop(0, TILES // COLUMNS, columns, 0)

    pl.run_scoped(
        products,
        tuple(pltpu.ACC(0)((256, 256), F32) for _ in range(2)),
        tuple(pltpu.ACC(1)((256, 256), F32) for _ in range(2)),
        tuple(pltpu.ACC(0)((64, 256), F32) for _ in range(COLUMNS)),
        tuple(pltpu.ACC(1)((32, 256), F32) for _ in range(COLUMNS)),
    )

    def gather(accs, by_matmul, by_permute):
        for u, (p, q) in enumerate(by_matmul):
            index = jnp.concatenate([conn_ref[p : p + 1, :], conn_ref[q : q + 1, :]], axis=1)
            selected(accs, t3_ref, index.astype(F32), 16, u)
        for p in by_permute:
            for r, value in enumerate(permuted(tab_ref, conn_ref[p : p + 1, :], 16)):
                gat_ref[p * 32 + r * 8 : p * 32 + r * 8 + 8, :] = value
        for u, (p, q) in enumerate(by_matmul):
            parts = pltpu.matmul_pop(accs[u])
            value = parts[0:32] + parts[32:64] + parts[64:96]
            gat_ref[p * 32 : p * 32 + 32, :] = value[:, 0:128]
            gat_ref[q * 32 : q * 32 + 32, :] = value[:, 128:256]

    chord_points = [p for p in range(64) if (p // 4) % 4 in (0, 3)]
    span_points = [p for p in range(64) if p not in chord_points and p % 4 in (0, 3)]
    inside = [p for p in range(64) if p not in chord_points + span_points]

    def gather_stage(points, count):
        pairs = [(points[2 * u], points[2 * u + 1]) for u in range(count)]

        def scoped(*accs):
            for acc in accs:
                pltpu.matmul_pop(acc)
            gather(accs, pairs, points[2 * count :])

        pl.run_scoped(scoped, *[pltpu.ACC(u % 2)((96, 256), F32) for u in range(count)])

    gather_stage(chord_points, 8)

    derivative = lobatto_derivative()

    def rows(first, p):
        return gat_ref[pl.ds(p * 32 + first, 5, stride=3), :]

    def jacobian(p, directions):
        a, b, c = p // 16, (p // 4) % 4, p % 4
        lines = (
            (a, [k * 16 + b * 4 + c for k in range(4)]),
            (b, [a * 16 + k * 4 + c for k in range(4)]),
            (c, [a * 16 + b * 4 + k for k in range(4)]),
        )
        jac = [[None] * 3 for _ in range(3)]
        for i in range(3):
            for d in directions:
                at, points = lines[d]
                terms = [
                    float(derivative[at, k]) * rows(i, q)
                    for k, q in enumerate(points)
                    if derivative[at, k] != 0.0
                ]
                jac[i][d] = functools.reduce(jnp.add, terms)
        return jac

    def metric(jac, d, i):
        i1, i2, d1, d2 = (i + 1) % 3, (i + 2) % 3, (d + 1) % 3, (d + 2) % 3
        return jac[i1][d1] * jac[i2][d2] - jac[i1][d2] * jac[i2][d1]

    def normal(entries, speed):
        return entries[0] * speed[0] + entries[1] * speed[1] + entries[2] * speed[2]

    def face_flux(p, d):
        jac = jacobian(p, [k for k in range(3) if k != d])
        speed = [rows(15 + i, p) for i in range(3)]
        fl_ref[d - 1, p, 0:5, :] = normal([metric(jac, d, i) for i in range(3)], speed)

    def metrics(p):
        jac = jacobian(p, range(3))
        speed = [rows(15 + i, p) for i in range(3)]
        entries = [[metric(jac, d, i) for i in range(3)] for d in range(3)]
        det_ref[:, p, :] = (
            jac[0][0] * entries[0][0] + jac[0][1] * entries[1][0] + jac[0][2] * entries[2][0]
        )
        for d in range(3):
            flux_ref[:, d, p, :] = normal(entries[d], speed)

    lane = lax.broadcasted_iota(jnp.int32, (8, 128), 1)

    def quarters(values):
        out = values[0]
        for q in range(1, 4):
            out = jnp.where(lane >= q * 32, values[q], out)
        return out

    across = {0: (beside[1], 1), 1: (beside[0], 0), 2: (beside[3], 3), 3: (beside[2], 2)}

    def trace(t):
        index = jnp.broadcast_to(
            jnp.concatenate([elem_ref[t : t + 1, :]] * 4, axis=1), (8, 128)
        )
        for a in range(4):
            if t < 2:
                points = [a * 16 + q * 4 + 3 * t for q in range(4)]
            else:
                points = [a * 16 + 12 * (t - 2) + q for q in range(4)]
            picked = quarters(
                [
                    jnp.take_along_axis(
                        fl_ref[1 - t // 2, p], index, axis=1, mode="promise_in_bounds"
                    )
                    for p in points
                ]
            )
            tr_ref[t, a] = picked if t % 2 else -picked

    def send(t):
        device, slot = across[t]
        pltpu.make_async_remote_copy(
            src_ref=tr_ref.at[t],
            dst_ref=rc_ref.at[slot],
            send_sem=sems.at[9],
            recv_sem=sems.at[10],
            device_id=device,
            device_id_type=MESH,
        ).start()

    fl_ref[...] = jnp.zeros_like(fl_ref)
    for p in chord_points:
        face_flux(p, 1)
    for t in (2, 3):
        trace(t)
    for t in (2, 3):
        send(t)
    gather_stage(span_points, 4)
    for p in range(64):
        if p % 4 in (0, 3):
            face_flux(p, 2)
    for t in (0, 1):
        trace(t)
    for t in (0, 1):
        send(t)
    gather_stage(inside, 4)
    for p in range(64):
        metrics(p)
    stores = [
        pltpu.make_async_copy(det_ref, det_out, store.at[0]),
        pltpu.make_async_copy(flux_ref, flux_out, store.at[1]),
    ]
    for copy in stores:
        copy.start()
    every6 = pltpu.make_async_remote_copy(
        src_ref=tr_ref,
        dst_ref=rc_ref,
        send_sem=sems.at[9],
        recv_sem=sems.at[10],
        device_id=partner,
        device_id_type=MESH,
    )
    every6.wait_recv()
    every6.wait_send()

    for t in range(4):
        index = jnp.broadcast_to(
            jnp.concatenate([match_ref[t : t + 1, :] + 32 * q for q in range(4)], axis=1), (8, 128)
        )
        for a in range(4):
            own = tr_ref[t, a]
            other = jnp.take_along_axis(rc_ref[t, a], index, axis=1, mode="promise_in_bounds")
            if t == 0:
                other = jnp.where(jnp.broadcast_to(span == 0, (8, 128)), -own, other)
            if t == 1:
                other = jnp.where(
                    jnp.broadcast_to(span == NY * NCORE - 1, (8, 128)), -own, other
                )
            face_ref[t, a] = 0.5 * (own - other)
    for copy in stores:
        copy.wait()


def finish(
    det_in,
    flux_in,
    packed_in,
    det_out,
    flux_out,
    face_out,
    det_ref,
    flux_ref,
    packed_ref,
    face_ref,
    sem,
):
    pairs = ((det_in, det_ref, det_out), (flux_in, flux_ref, flux_out))
    packed = pltpu.make_async_copy(packed_in, packed_ref, sem.at[5])
    packed.start()
    loads = [pltpu.make_async_copy(a, b, sem.at[k]) for k, (a, b, _) in enumerate(pairs)]
    stores = [pltpu.make_async_copy(b, c, sem.at[k + 2]) for k, (_, b, c) in enumerate(pairs)]
    for copy in loads:
        copy.start()
    for k in range(2):
        loads[k].wait()
        stores[k].start()
    packed.wait()
    for t in range(4):
        for a in range(4):
            value = packed_ref[t, a]
            for q in range(4):
                face_ref[t, :, a * 4 + q, :] = value[0:5, q * 32 : (q + 1) * 32]
    stores.append(pltpu.make_async_copy(face_ref, face_out, sem.at[4]))
    stores[2].start()
    for copy in stores:
        copy.wait()


def on_device(
    node_pos, ctrl_pos, ctrl_ids, wing_shift, wing_speed, minv, conn, face_elem, face_match
):
    vmem = pl.BlockSpec(memory_space=pltpu.VMEM)
    hbm = pl.BlockSpec(memory_space=pltpu.HBM)
    dma = pltpu.SemaphoreType.DMA
    det, flux, packed = pl.pallas_call(
        kernel,
        out_shape=(
            jax.ShapeDtypeStruct((5, 64, 128), F32),
            jax.ShapeDtypeStruct((5, 3, 64, 128), F32),
            jax.ShapeDtypeStruct((4, 4, 8, 128), F32),
        ),
        in_specs=[hbm] * 10,
        out_specs=[hbm, hbm, vmem],
        scratch_shapes=[
            pltpu.VMEM((1, 32), jnp.int32),
            pltpu.VMEM((3, 32), F32),
            pltpu.VMEM((3, 2048), F32),
            pltpu.VMEM((15, 1024), F32),
            pltpu.VMEM((15, 1024), F32),
            pltpu.VMEM((32, 8192), F32),
            pltpu.VMEM((64, 128), jnp.int32),
            pltpu.VMEM((4, 32), jnp.int32),
            pltpu.VMEM((4, 32), jnp.int32),
            pltpu.VMEM((4, 384, 256), BF16),
            pltpu.VMEM((5, 64, 128), F32),
            pltpu.VMEM((5, 3, 64, 128), F32),
            pltpu.VMEM((1, 1, 128), F32),
            pltpu.VMEM((DEVICES, 1, 128), F32),
            pltpu.VMEM((DEVICES, 8, 128), F32),
            pltpu.VMEM((DEVICES, 128), F32),
            pltpu.VMEM((64, 128), F32),
            pltpu.VMEM((96, 1024), BF16),
            pltpu.VMEM((32, 1024), F32),
            pltpu.VMEM((96, 8192), BF16),
            pltpu.VMEM((96, 8192), BF16),
            pltpu.VMEM((96, 256), F32),
            pltpu.VMEM((32, 128), F32),
            pltpu.VMEM((32, DEVICES), F32),
            pltpu.VMEM((32, 64, DEVICES), BF16),
            pltpu.VMEM((STORED, TILES, 256, 256), BF16),
            pltpu.VMEM((STORED, TILES, 256, 256), BF16),
            pltpu.VMEM((2, DEVICES, 256), BF16),
            pltpu.VMEM((4, DEVICES, 256), BF16),
            pltpu.VMEM((32, 2048), BF16),
            pltpu.VMEM((96, 2048), BF16),
            pltpu.VMEM((32, 2048), F32),
            pltpu.VMEM((64 * 32, 128), F32),
            pltpu.VMEM((2, 64, 8, 128), F32),
            pltpu.VMEM((4, 4, 8, 128), F32),
            pltpu.VMEM((4, 4, 8, 128), F32),
            dma((12,)),
            dma((7,)),
            dma((10,)),
            dma((2,)),
        ],
        compiler_params=pltpu.CompilerParams(
            collective_id=0, has_side_effects=True, vmem_limit_bytes=67043328
        ),
        name="wing",
    )(
        ctrl_ids.reshape(1, 32),
        ctrl_pos,
        node_pos,
        wing_shift,
        wing_speed,
        minv,
        conn,
        face_elem.reshape(4, 32),
        face_match.reshape(4, 32),
        selection(),
    )
    det, flux, face = pl.pallas_call(
        finish,
        out_shape=(
            jax.ShapeDtypeStruct((5, 64, 128), F32),
            jax.ShapeDtypeStruct((5, 3, 64, 128), F32),
            jax.ShapeDtypeStruct((4, 5, 16, 32), F32),
        ),
        in_specs=[hbm] * 3,
        out_specs=[hbm] * 3,
        scratch_shapes=[
            pltpu.VMEM((5, 64, 128), F32),
            pltpu.VMEM((5, 3, 64, 128), F32),
            pltpu.VMEM((4, 4, 8, 128), F32),
            pltpu.VMEM((4, 5, 16, 32), F32),
            dma((6,)),
        ],
        name="wing_end",
    )(det, flux, packed)
    return det, flux, face.reshape(1, 1, 4, 5, 16, 32)


def solution(mesh):
    split = Mesh(mesh.devices.reshape(NY, NCORE, NZ, NX), SPAN_CHORD)
    return jax.shard_map(
        on_device,
        mesh=split,
        in_specs=(
            P(None, SPAN_CHORD),
            P(None, SPAN_CHORD),
            P(SPAN_CHORD),
            P(),
            P(),
            P(SPAN_CHORD, None),
            P(None, SPAN_CHORD),
            P(SPAN, CHORD, None, None),
            P(SPAN, CHORD, None, None),
        ),
        out_specs=(
            P(None, None, SPAN_CHORD),
            P(None, None, None, SPAN_CHORD),
            P(SPAN, CHORD, None, None, None, None),
        ),
        check_vma=False,
    )
```

```python
import functools

import jax
import jax.numpy as jnp
import numpy as np
from jax import lax
from jax.experimental import pallas as pl
from jax.experimental.pallas import tpu as pltpu
from jax.sharding import Mesh
from jax.sharding import PartitionSpec as P

SPAN_CHORD = ("y", "core", "z", "x")
SPAN = ("y", "core")
CHORD = ("z", "x")
NY, NCORE, NZ, NX = 4, 2, 8, 4
DEVICES = NY * NCORE * NZ * NX
GROUP = NCORE * NZ
MESH = pl.DeviceIdType.MESH
F32 = jnp.float32
BF16 = jnp.bfloat16

WIDTH = 0.1
HALF_INV = 1.0 / (2.0 * WIDTH**2)
CROSS = float(2.0 * HALF_INV * np.log2(np.e))
STORED = 24
TILES = 8
COLUMNS = 2
R_PERMUTED = 32
R_UNITS = (64 - R_PERMUTED) // 2


PAIRS = ((0, 0), (0, 1), (0, 2), (1, 0), (1, 1), (2, 0))


def selection():
    chosen = np.zeros((4, 384, 256), np.float32)
    for g in range(4):
        for l in range(8):
            for j, (part, _) in enumerate(PAIRS):
                for k in range(3):
                    chosen[g, part * 128 + 32 * (k + 1) + 8 * g + l, l * 32 + 3 * j + k] = 1.0
    return jnp.asarray(chosen, BF16)


def lobatto_derivative():
    points = np.array([-1.0, -1.0 / np.sqrt(5.0), 1.0 / np.sqrt(5.0), 1.0])
    barycentric = np.array(
        [
            1.0 / np.prod([points[t] - points[s] for s in range(4) if s != t])
            for t in range(4)
        ]
    )
    derivative = np.zeros((4, 4))
    for t in range(4):
        for s in range(4):
            if s != t:
                derivative[t, s] = barycentric[s] / barycentric[t] / (points[t] - points[s])
        derivative[t, t] = -np.sum(derivative[t])
    return derivative


def split3(value):
    high = value.astype(BF16)
    rest = value - high.astype(F32)
    middle = rest.astype(BF16)
    low = (rest - middle.astype(F32)).astype(BF16)
    return high, middle, low


def one_hot(index, blocks):
    width = index.shape[1]
    block = jnp.floor(index * (1.0 / 128.0))
    lane = (index - block * 128.0).astype(BF16)
    block = jnp.broadcast_to(block.astype(BF16), (128, width))
    row = lax.broadcasted_iota(jnp.int32, (128, width), 0).astype(F32).astype(BF16)
    one = jnp.ones((128, width), BF16)
    zero = jnp.zeros((128, width), BF16)
    inner = jnp.where(row == jnp.broadcast_to(lane, (128, width)), one, zero)
    return jnp.concatenate(
        [jnp.where(block == jnp.full((128, width), b, BF16), inner, zero) for b in range(blocks)],
        axis=0,
    )


def kernel(
    ids_in,
    ctrl_in,
    nodes_in,
    shift_in,
    speed_in,
    minv_in,
    conn_in,
    elem_in,
    match_in,
    sel_in,
    det_out,
    flux_out,
    face_ref,
    ids_ref,
    ctrl_ref,
    nodes_ref,
    shift_ref,
    speed_ref,
    minv_ref,
    conn_ref,
    elem_ref,
    match_ref,
    sel_ref,
    det_ref,
    flux_ref,
    own_ref,
    g1_ref,
    g2_ref,
    gp_ref,
    idr_ref,
    table_ref,
    plain_ref,
    r3_ref,
    m3_ref,
    cross_ref,
    wt_ref,
    scale_ref,
    wc_ref,
    kh_ref,
    kl_ref,
    parts_ref,
    lhs_ref,
    nb_ref,
    t3_ref,
    tab_ref,
    gat_ref,
    fl_ref,
    tr_ref,
    rc_ref,
    sems,
    recv3,
    load,
    store,
):
    y, core, z, x = (lax.axis_index(name) for name in SPAN_CHORD)
    group = y * NX + x
    place = core * NZ + z
    line = [(dc, dz) for dc in range(NCORE) for dz in range(NZ) if (dc, dz) != (0, 0)]
    plane = [(dy, dx) for dy in range(NY) for dx in range(NX) if (dy, dx) != (0, 0)]

    near = [dy != 2 and dx != 2 for dy, dx in plane]

    def line_device(dc, dz):
        return (y, lax.rem(core + dc, NCORE), lax.rem(z + dz, NZ), x)

    def plane_device(dy, dx):
        return (lax.rem(y + dy, NY), core, z, lax.rem(x + dx, NX))

    span = y * NCORE + core
    chord = z * NX + x

    def span_device(step):
        j = lax.rem(span + step + NY * NCORE, NY * NCORE)
        return (j // NCORE, lax.rem(j, NCORE), z, x)

    def chord_device(step):
        k = lax.rem(chord + step + NZ * NX, NZ * NX)
        return (y, core, k // NX, lax.rem(k, NX))

    partner = (y, 1 - core, z, x)
    beside = [span_device(1), span_device(-1), chord_device(1), chord_device(-1)]

    barrier = pltpu.get_barrier_semaphore()
    greeted = [line_device(*d) for d in line] + [plane_device(*d) for d in plane] + beside
    for device in greeted:
        pl.semaphore_signal(barrier, inc=1, device_id=device, device_id_type=MESH)

    loads = [
        pltpu.make_async_copy(source, target, load.at[k])
        for k, (source, target) in enumerate(
            (
                (ids_in, ids_ref),
                (ctrl_in, ctrl_ref),
                (shift_in, shift_ref),
                (speed_in, speed_ref),
                (minv_in, minv_ref),
                (nodes_in, nodes_ref),
                (conn_in, conn_ref),
                (elem_in, elem_ref),
                (match_in, match_ref),
                (sel_in, sel_ref),
            )
        )
    ]
    for copy in loads:
        copy.start()
    for copy in loads[:2]:
        copy.wait()
    own_ref[0] = jnp.concatenate(
        [ids_ref[...].astype(F32)] + [ctrl_ref[k : k + 1, :] for k in range(3)], axis=1
    )
    g1_ref[group * GROUP + place] = own_ref[0]
    pl.semaphore_wait(barrier, len(greeted))

    def first_copy(k, device):
        return pltpu.make_async_remote_copy(
            src_ref=own_ref,
            dst_ref=g1_ref.at[pl.ds(group * GROUP + place, 1)],
            send_sem=sems.at[0],
            recv_sem=sems.at[1],
            device_id=device,
            device_id_type=MESH,
        )

    copies1 = [first_copy(k, line_device(*d)) for k, d in enumerate(line)]
    for copy in copies1:
        copy.start()
    def all_rows(ref, count, sent, received):
        return pltpu.make_async_remote_copy(
            src_ref=ref.at[pl.ds(0, count)],
            dst_ref=ref.at[pl.ds(0, count)],
            send_sem=sems.at[sent],
            recv_sem=sems.at[received],
            device_id=partner,
            device_id_type=MESH,
        )

    every1 = all_rows(g1_ref, len(line), 0, 1)
    every2 = all_rows(g1_ref, len(plane) * GROUP, 2, 3)
    every1.wait_recv()

    def second_copy(k, device):
        rows = pl.ds(group * GROUP, GROUP)
        return pltpu.make_async_remote_copy(
            src_ref=g1_ref.at[rows],
            dst_ref=g1_ref.at[rows],
            send_sem=sems.at[2],
            recv_sem=sems.at[3],
            device_id=device,
            device_id_type=MESH,
        )

    copies2 = [second_copy(k, plane_device(*d)) for k, d in enumerate(plane)]
    for copy in copies2:
        copy.start()
    for copy in loads[2:]:
        copy.wait()
    table = jnp.concatenate(
        [shift_ref[...], speed_ref[...], jnp.zeros((2, shift_ref.shape[1]), F32)], axis=0
    )
    plain_ref[...] = table
    for k, part in enumerate(split3(table)):
        table_ref[k * 32 : (k + 1) * 32, :] = part
    for k, part in enumerate(split3(minv_ref[...])):
        m3_ref[k * 32 : (k + 1) * 32, :] = part
    node_parts = split3(nodes_ref[...] * CROSS)
    nb_ref[...] = jnp.concatenate(
        [node_parts[part].astype(F32) for _, part in PAIRS] + [jnp.zeros((14, 2048), F32)], axis=0
    ).astype(BF16)
    every1.wait_send()
    every2.wait_recv()
    every2.wait_send()

    gp_ref[...] = g1_ref[...].reshape(DEVICES, 128)
    for ny in range(NY):
        idr_ref[ny * GROUP : (ny + 1) * GROUP, :] = jnp.concatenate(
            [gp_ref[(ny * NX + q) * GROUP : (ny * NX + q + 1) * GROUP, 0:32] for q in range(NX)],
            axis=1,
        )

    def permuted(source_ref, index, blocks):
        node = jnp.broadcast_to(index, (8, 128))
        lane = node & 127
        block = node >> 7
        found = [None] * 4
        for k in range(blocks):
            here = block == k
            for r in range(4):
                taken = jnp.take_along_axis(
                    source_ref[r * 8 : r * 8 + 8, k * 128 : (k + 1) * 128],
                    lane,
                    axis=1,
                    mode="promise_in_bounds",
                )
                found[r] = taken if k == 0 else jnp.where(here, taken, found[r])
        return found

    def selected(accs, parts_ref, index, blocks, which):
        spread = one_hot(index, blocks)
        for k in range(blocks // 2):
            pltpu.matmul_push_rhs(
                spread[k * 256 : (k + 1) * 256], staging_register=0, mxu_index=which % 2
            )
            pltpu.matmul_acc_lhs(
                accs[which], parts_ref[:, k * 256 : (k + 1) * 256], load_staged_rhs=0
            )

    def first_stage(*accs):
        for acc in accs:
            pltpu.matmul_pop(acc)

        def right_side(i):
            for u in range(R_UNITS):
                pair = idr_ref[pl.ds((i * R_UNITS + u) * 2, 2), :]
                index = jnp.concatenate([pair[0:1], pair[1:2]], axis=1)
                selected(accs, table_ref, index, 8, u)
            for v in range(R_PERMUTED):
                row = 64 - R_PERMUTED + i * (R_PERMUTED) + v
                lanes = pl.ds(pl.multiple_of(row * 128, 128), 128)
                found = permuted(plain_ref, idr_ref[pl.ds(row, 1), :].astype(jnp.int32), 8)
                for k, part in enumerate(split3(jnp.concatenate(found, axis=0))):
                    r3_ref[k * 32 : (k + 1) * 32, lanes] = part
            for u in range(R_UNITS):
                lanes = pl.ds(pl.multiple_of((i * R_UNITS + u) * 256, 256), 256)
                r3_ref[:, lanes] = pltpu.matmul_pop(accs[u]).astype(BF16)

        right_side(0)

        for k in range(32):
            lanes = slice(k * 256, (k + 1) * 256)
            pltpu.matmul_push_rhs(
                jnp.concatenate([r3_ref[:, lanes], jnp.zeros((160, 256), BF16)], axis=0),
                staging_register=0,
                mxu_index=k % 2,
                transpose=True,
            )
            pltpu.matmul_acc_lhs(accs[k % 2], m3_ref[:, lanes], load_staged_rhs=0)
        cross_ref[...] = pltpu.matmul_pop(accs[0]) + pltpu.matmul_pop(accs[1])

    pl.run_scoped(first_stage, *[pltpu.ACC(u % 2)((96, 256), F32) for u in range(R_UNITS)])
    cross = cross_ref[...]

    def piece(a, b):
        return cross[a * 32 : (a + 1) * 32, b * 32 : (b + 1) * 32]

    weights = piece(0, 0) + (
        (piece(0, 1) + piece(1, 0)) + (piece(1, 1) + (piece(0, 2) + piece(2, 0)))
    )
    wt_ref[:, 0:32] = weights
    mine = group * GROUP + place
    g2_ref[mine] = jnp.concatenate(
        [wt_ref[pl.ds(q, 8, stride=4), 0:32] for q in range(4)], axis=1
    )

    def third_copy(k, device):
        return pltpu.make_async_remote_copy(
            src_ref=g2_ref.at[pl.ds(mine, 1)],
            dst_ref=g2_ref.at[pl.ds(mine, 1)],
            send_sem=sems.at[4],
            recv_sem=recv3.at[k],
            device_id=device,
            device_id_type=MESH,
        )

    copies3 = [third_copy(k, line_device(0, k + 1)) for k in range(NZ - 1)]
    for copy in copies3:
        copy.start()

    def block_rows(of_y, of_x, of_core):
        return pl.ds((of_y * NX + of_x) * GROUP + of_core * NZ, NZ)

    def fourth_copy(k, device, rows):
        return pltpu.make_async_remote_copy(
            src_ref=g2_ref.at[rows],
            dst_ref=g2_ref.at[rows],
            send_sem=sems.at[5],
            recv_sem=sems.at[6 if near[k] else 11],
            device_id=device,
            device_id_type=MESH,
        )

    def forward(step):
        row = group * GROUP + core * NZ + lax.rem(z + NZ - step, NZ)
        for k, d in enumerate(plane):
            fourth_copy(k, plane_device(*d), pl.ds(row, 1)).start()

    forward(0)

    def parts_of(value):
        high = value.astype(BF16)
        return high, (value - high.astype(F32)).astype(BF16)

    def cross_rhs(l, lanes):
        pieces = [nb_ref[:, lanes]]
        if l > 0:
            pieces = [jnp.zeros((32 * l, 256), BF16)] + pieces
        if l < 7:
            pieces = pieces + [jnp.zeros((32 * (7 - l), 256), BF16)]
        return jnp.concatenate(pieces, axis=0)

    def generate(accs):
        def step(t, carry):
            lanes = pl.ds(pl.multiple_of(t * 256, 256), 256)
            for l in range(8):
                used = [accs[l % 2][(l // 2 * 3 + g) % 4] for g in range(3)]
                pltpu.matmul_push_rhs(cross_rhs(l, lanes), staging_register=0, mxu_index=l % 2)
                for g in range(3):
                    pltpu.matmul_acc_lhs(
                        used[g], lhs_ref[g], load_staged_rhs=0 if g == 0 else None
                    )
                for g in range(3):
                    high, low = parts_of(jnp.exp2(pltpu.matmul_pop(used[g])))
                    kh_ref[g * 8 + l, t] = high
                    kl_ref[g * 8 + l, t] = low
            return carry

        return step

    def start_generation(*accs):
        for acc in accs:
            pltpu.matmul_pop(acc)
        for g in range(4):
            for k in range(2):
                chosen = sel_ref[g, k * 256 : min((k + 1) * 256, 384), :]
                if k == 1:
                    chosen = jnp.concatenate([chosen, jnp.zeros((128, 256), BF16)], axis=0)
                pltpu.matmul_push_rhs(chosen, staging_register=0, mxu_index=g % 2)
                pltpu.matmul_acc_lhs(accs[g], parts_ref[k], load_staged_rhs=0)
        for g in range(4):
            lhs_ref[g] = pltpu.matmul_pop(accs[g]).astype(BF16)

    def generate_range(first, last):
        def scoped(zero, one):
            for acc in (*zero, *one):
                pltpu.matmul_pop(acc)
            lax.fori_loop(first, last, generate((zero, one)), 0)

        pl.run_scoped(
            scoped,
            tuple(pltpu.ACC(0)((256, 256), F32) for _ in range(4)),
            tuple(pltpu.ACC(1)((256, 256), F32) for _ in range(4)),
        )

    for k, part in enumerate(split3(gp_ref[...])):
        parts_ref[k // 2, :, (k % 2) * 128 : (k % 2 + 1) * 128] = part
    parts_ref[1, :, 128:256] = jnp.zeros((DEVICES, 128), BF16)
    pl.run_scoped(start_generation, *[pltpu.ACC(g % 2)((256, 256), F32) for g in range(4)])

    generate_range(0, 2)

    for step in (1, 7, 2, 6):
        copies3[step - 1].wait_recv()
        forward(step)
    generate_range(2, 3)
    for step in (3, 5, 4):
        copies3[step - 1].wait_recv()
        forward(step)
    every3 = all_rows(g2_ref, NZ - 1, 4, 4)
    every4 = all_rows(g2_ref, NZ * len(plane), 5, 6)
    every5 = all_rows(g2_ref, NZ * NX * NY, 7, 8)

    def fifth_copy(k, dy, dx):
        rows = block_rows(lax.rem(y + NY - dy, NY), lax.rem(x + NX - dx, NX), core)
        return pltpu.make_async_remote_copy(
            src_ref=g2_ref.at[rows],
            dst_ref=g2_ref.at[rows],
            send_sem=sems.at[7],
            recv_sem=sems.at[8],
            device_id=partner,
            device_id_type=MESH,
        )

    copies5 = [fifth_copy(k, *d) for k, d in enumerate([(0, 0)] + plane)]
    copies5[0].start()
    every3.wait_send()
    generate_range(3, 6)
    all_rows(g2_ref, NZ * sum(near), 5, 6).wait_recv()
    for copy, close in zip(copies5[1:], near):
        if close:
            copy.start()
    generate_range(6, 7)
    all_rows(g2_ref, NZ * (len(near) - sum(near)), 5, 11).wait_recv()
    for copy, close in zip(copies5[1:], near):
        if not close:
            copy.start()
    every4.wait_send()
    generate_range(7, 8)
    turned = gp_ref[...].T
    scale_ref[...] = jnp.exp(
        -HALF_INV * (turned[32:64] ** 2 + turned[64:96] ** 2 + turned[96:128] ** 2)
    )
    every5.wait_recv()
    every5.wait_send()

    for j in range(8):
        block = g2_ref[:, j, :].T
        for q in range(4):
            l = 4 * j + q
            value = block[q * 32 : (q + 1) * 32] * scale_ref[l : l + 1, :]
            high = value.astype(BF16)
            wc_ref[l, 0:32, :] = high
            wc_ref[l, 32:64, :] = (value - high.astype(F32)).astype(BF16)

    def products(zero, one, high_accs, low_accs):
        accs = (zero, one)
        for acc in (*zero, *one, *high_accs, *low_accs):
            pltpu.matmul_pop(acc)

        turn = [0, 0]

        def multiply(mxu, acc, lhs, rhs):
            register = turn[mxu] % 2
            turn[mxu] += 1
            pltpu.matmul_push_rhs(rhs, staging_register=register, mxu_index=mxu)
            pltpu.matmul_acc_lhs(acc, lhs, load_staged_rhs=register)

        def add(u, l, high, low):
            multiply(0, high_accs[u], wc_ref[l], high)
            multiply(1, low_accs[u], wc_ref[l, 0:32], low)

        def columns(i, carry):
            lanes = [
                pl.ds(pl.multiple_of((COLUMNS * i + u) * 256, 256), 256) for u in range(COLUMNS)
            ]

            def power(n):
                u, l = n // 8, n % 8
                multiply(n % 2, accs[n % 2][(n // 2) % 2], lhs_ref[3], cross_rhs(l, lanes[u]))

            power(0)
            power(1)
            def stored(n):
                u, l = n // 8, n % 8
                t = COLUMNS * i + u
                for k in range(3 * l, 3 * l + 3):
                    add(u, k, kh_ref[k, t], kl_ref[k, t])

            for n in range(8 * COLUMNS):
                u, l = n // 8, n % 8
                value = jnp.exp2(pltpu.matmul_pop(accs[n % 2][(n // 2) % 2]))
                if n < 8 * COLUMNS - 2:
                    power(n + 2)
                stored(n)
                add(u, 24 + l, *parts_of(value))
            for u in range(COLUMNS):
                first = pltpu.matmul_pop(high_accs[u])
                total = first[0:32] + first[32:64] + pltpu.matmul_pop(low_accs[u])
                place_of = nodes_ref[:, lanes[u]]
                factor = jnp.exp(
                    -HALF_INV * jnp.sum(place_of * place_of, axis=0, keepdims=True)
                )
                base = jnp.concatenate([place_of] * 5 + [jnp.zeros((17, 256), F32)], axis=0)
                moved = total * factor + base
                tab_ref[:, lanes[u]] = moved
                for k, part in enumerate(split3(moved)):
                    t3_ref[k * 32 : (k + 1) * 32, lanes[u]] = part
            return carry

        lax.fori_loop(0, TILES // COLUMNS, columns, 0)

    pl.run_scoped(
        products,
        tuple(pltpu.ACC(0)((256, 256), F32) for _ in range(2)),
        tuple(pltpu.ACC(1)((256, 256), F32) for _ in range(2)),
        tuple(pltpu.ACC(0)((64, 256), F32) for _ in range(COLUMNS)),
        tuple(pltpu.ACC(1)((32, 256), F32) for _ in range(COLUMNS)),
    )

    def gather(accs, by_matmul, by_permute):
        for u, (p, q) in enumerate(by_matmul):
            index = jnp.concatenate([conn_ref[p : p + 1, :], conn_ref[q : q + 1, :]], axis=1)
            selected(accs, t3_ref, index.astype(F32), 16, u)
        for p in by_permute:
            for r, value in enumerate(permuted(tab_ref, conn_ref[p : p + 1, :], 16)):
                gat_ref[p * 32 + r * 8 : p * 32 + r * 8 + 8, :] = value
        for u, (p, q) in enumerate(by_matmul):
            parts = pltpu.matmul_pop(accs[u])
            value = parts[0:32] + parts[32:64] + parts[64:96]
            gat_ref[p * 32 : p * 32 + 32, :] = value[:, 0:128]
            gat_ref[q * 32 : q * 32 + 32, :] = value[:, 128:256]

    chord_points = [p for p in range(64) if (p // 4) % 4 in (0, 3)]
    span_points = [p for p in range(64) if p not in chord_points and p % 4 in (0, 3)]
    inside = [p for p in range(64) if p not in chord_points + span_points]

    def gather_stage(points, count):
        pairs = [(points[2 * u], points[2 * u + 1]) for u in range(count)]

        def scoped(*accs):
            for acc in accs:
                pltpu.matmul_pop(acc)
            gather(accs, pairs, points[2 * count :])

        pl.run_scoped(scoped, *[pltpu.ACC(u % 2)((96, 256), F32) for u in range(count)])

    gather_stage(chord_points, 8)

    derivative = lobatto_derivative()

    def rows(first, p):
        return gat_ref[pl.ds(p * 32 + first, 5, stride=3), :]

    def jacobian(p, directions):
        a, b, c = p // 16, (p // 4) % 4, p % 4
        lines = (
            (a, [k * 16 + b * 4 + c for k in range(4)]),
            (b, [a * 16 + k * 4 + c for k in range(4)]),
            (c, [a * 16 + b * 4 + k for k in range(4)]),
        )
        jac = [[None] * 3 for _ in range(3)]
        for i in range(3):
            for d in directions:
                at, points = lines[d]
                terms = [
                    float(derivative[at, k]) * rows(i, q)
                    for k, q in enumerate(points)
                    if derivative[at, k] != 0.0
                ]
                jac[i][d] = functools.reduce(jnp.add, terms)
        return jac

    def metric(jac, d, i):
        i1, i2, d1, d2 = (i + 1) % 3, (i + 2) % 3, (d + 1) % 3, (d + 2) % 3
        return jac[i1][d1] * jac[i2][d2] - jac[i1][d2] * jac[i2][d1]

    def normal(entries, speed):
        return entries[0] * speed[0] + entries[1] * speed[1] + entries[2] * speed[2]

    def face_flux(p, d):
        jac = jacobian(p, [k for k in range(3) if k != d])
        speed = [rows(15 + i, p) for i in range(3)]
        fl_ref[d - 1, p, 0:5, :] = normal([metric(jac, d, i) for i in range(3)], speed)

    def metrics(p):
        jac = jacobian(p, range(3))
        speed = [rows(15 + i, p) for i in range(3)]
        entries = [[metric(jac, d, i) for i in range(3)] for d in range(3)]
        det_ref[:, p, :] = (
            jac[0][0] * entries[0][0] + jac[0][1] * entries[1][0] + jac[0][2] * entries[2][0]
        )
        for d in range(3):
            flux_ref[:, d, p, :] = normal(entries[d], speed)

    lane = lax.broadcasted_iota(jnp.int32, (8, 128), 1)

    def quarters(values):
        out = values[0]
        for q in range(1, 4):
            out = jnp.where(lane >= q * 32, values[q], out)
        return out

    across = {0: (beside[1], 1), 1: (beside[0], 0), 2: (beside[3], 3), 3: (beside[2], 2)}

    def trace(t):
        index = jnp.broadcast_to(
            jnp.concatenate([elem_ref[t : t + 1, :]] * 4, axis=1), (8, 128)
        )
        for a in range(4):
            if t < 2:
                points = [a * 16 + q * 4 + 3 * t for q in range(4)]
            else:
                points = [a * 16 + 12 * (t - 2) + q for q in range(4)]
            picked = quarters(
                [
                    jnp.take_along_axis(
                        fl_ref[1 - t // 2, p], index, axis=1, mode="promise_in_bounds"
                    )
                    for p in points
                ]
            )
            tr_ref[t, a] = picked if t % 2 else -picked

    def send(t):
        device, slot = across[t]
        pltpu.make_async_remote_copy(
            src_ref=tr_ref.at[t],
            dst_ref=rc_ref.at[slot],
            send_sem=sems.at[9],
            recv_sem=sems.at[10],
            device_id=device,
            device_id_type=MESH,
        ).start()

    fl_ref[...] = jnp.zeros_like(fl_ref)
    for p in chord_points:
        face_flux(p, 1)
    for t in (2, 3):
        trace(t)
    for t in (2, 3):
        send(t)
    gather_stage(span_points, 4)
    for p in range(64):
        if p % 4 in (0, 3):
            face_flux(p, 2)
    for t in (0, 1):
        trace(t)
    for t in (0, 1):
        send(t)
    gather_stage(inside, 4)
    for p in range(64):
        metrics(p)
    stores = [
        pltpu.make_async_copy(det_ref, det_out, store.at[0]),
        pltpu.make_async_copy(flux_ref, flux_out, store.at[1]),
    ]
    for copy in stores:
        copy.start()
    every6 = pltpu.make_async_remote_copy(
        src_ref=tr_ref,
        dst_ref=rc_ref,
        send_sem=sems.at[9],
        recv_sem=sems.at[10],
        device_id=partner,
        device_id_type=MESH,
    )
    every6.wait_recv()
    every6.wait_send()

    for t in range(4):
        index = jnp.broadcast_to(
            jnp.concatenate([match_ref[t : t + 1, :] + 32 * q for q in range(4)], axis=1), (8, 128)
        )
        for a in range(4):
            own = tr_ref[t, a]
            other = jnp.take_along_axis(rc_ref[t, a], index, axis=1, mode="promise_in_bounds")
            if t == 0:
                other = jnp.where(jnp.broadcast_to(span == 0, (8, 128)), -own, other)
            if t == 1:
                other = jnp.where(
                    jnp.broadcast_to(span == NY * NCORE - 1, (8, 128)), -own, other
                )
            face_ref[t, a] = 0.5 * (own - other)
    for copy in stores:
        copy.wait()


def finish(
    det_in,
    flux_in,
    packed_in,
    det_out,
    flux_out,
    face_out,
    det_ref,
    flux_ref,
    packed_ref,
    face_ref,
    sem,
):
    pairs = ((det_in, det_ref, det_out), (flux_in, flux_ref, flux_out))
    packed = pltpu.make_async_copy(packed_in, packed_ref, sem.at[5])
    packed.start()
    loads = [pltpu.make_async_copy(a, b, sem.at[k]) for k, (a, b, _) in enumerate(pairs)]
    stores = [pltpu.make_async_copy(b, c, sem.at[k + 2]) for k, (_, b, c) in enumerate(pairs)]
    for copy in loads:
        copy.start()
    for k in range(2):
        loads[k].wait()
        stores[k].start()
    packed.wait()
    for t in range(4):
        for a in range(4):
            value = packed_ref[t, a]
            for q in range(4):
                face_ref[t, :, a * 4 + q, :] = value[0:5, q * 32 : (q + 1) * 32]
    stores.append(pltpu.make_async_copy(face_ref, face_out, sem.at[4]))
    stores[2].start()
    for copy in stores:
        copy.wait()


def on_device(
    node_pos, ctrl_pos, ctrl_ids, wing_shift, wing_speed, minv, conn, face_elem, face_match
):
    vmem = pl.BlockSpec(memory_space=pltpu.VMEM)
    hbm = pl.BlockSpec(memory_space=pltpu.HBM)
    dma = pltpu.SemaphoreType.DMA
    det, flux, packed = pl.pallas_call(
        kernel,
        out_shape=(
            jax.ShapeDtypeStruct((5, 64, 128), F32),
            jax.ShapeDtypeStruct((5, 3, 64, 128), F32),
            jax.ShapeDtypeStruct((4, 4, 8, 128), F32),
        ),
        in_specs=[hbm] * 10,
        out_specs=[hbm, hbm, vmem],
        scratch_shapes=[
            pltpu.VMEM((1, 32), jnp.int32),
            pltpu.VMEM((3, 32), F32),
            pltpu.VMEM((3, 2048), F32),
            pltpu.VMEM((15, 1024), F32),
            pltpu.VMEM((15, 1024), F32),
            pltpu.VMEM((32, 8192), F32),
            pltpu.VMEM((64, 128), jnp.int32),
            pltpu.VMEM((4, 32), jnp.int32),
            pltpu.VMEM((4, 32), jnp.int32),
            pltpu.VMEM((4, 384, 256), BF16),
            pltpu.VMEM((5, 64, 128), F32),
            pltpu.VMEM((5, 3, 64, 128), F32),
            pltpu.VMEM((1, 1, 128), F32),
            pltpu.VMEM((DEVICES, 1, 128), F32),
            pltpu.VMEM((DEVICES, 8, 128), F32),
            pltpu.VMEM((DEVICES, 128), F32),
            pltpu.VMEM((64, 128), F32),
            pltpu.VMEM((96, 1024), BF16),
            pltpu.VMEM((32, 1024), F32),
            pltpu.VMEM((96, 8192), BF16),
            pltpu.VMEM((96, 8192), BF16),
            pltpu.VMEM((96, 256), F32),
            pltpu.VMEM((32, 128), F32),
            pltpu.VMEM((32, DEVICES), F32),
            pltpu.VMEM((32, 64, DEVICES), BF16),
            pltpu.VMEM((STORED, TILES, 256, 256), BF16),
            pltpu.VMEM((STORED, TILES, 256, 256), BF16),
            pltpu.VMEM((2, DEVICES, 256), BF16),
            pltpu.VMEM((4, DEVICES, 256), BF16),
            pltpu.VMEM((32, 2048), BF16),
            pltpu.VMEM((96, 2048), BF16),
            pltpu.VMEM((32, 2048), F32),
            pltpu.VMEM((64 * 32, 128), F32),
            pltpu.VMEM((2, 64, 8, 128), F32),
            pltpu.VMEM((4, 4, 8, 128), F32),
            pltpu.VMEM((4, 4, 8, 128), F32),
            dma((12,)),
            dma((7,)),
            dma((10,)),
            dma((2,)),
        ],
        compiler_params=pltpu.CompilerParams(
            collective_id=0, has_side_effects=True, vmem_limit_bytes=67043328
        ),
        name="wing",
    )(
        ctrl_ids.reshape(1, 32),
        ctrl_pos,
        node_pos,
        wing_shift,
        wing_speed,
        minv,
        conn,
        face_elem.reshape(4, 32),
        face_match.reshape(4, 32),
        selection(),
    )
    det, flux, face = pl.pallas_call(
        finish,
        out_shape=(
            jax.ShapeDtypeStruct((5, 64, 128), F32),
            jax.ShapeDtypeStruct((5, 3, 64, 128), F32),
            jax.ShapeDtypeStruct((4, 5, 16, 32), F32),
        ),
        in_specs=[hbm] * 3,
        out_specs=[hbm] * 3,
        scratch_shapes=[
            pltpu.VMEM((5, 64, 128), F32),
            pltpu.VMEM((5, 3, 64, 128), F32),
            pltpu.VMEM((4, 4, 8, 128), F32),
            pltpu.VMEM((4, 5, 16, 32), F32),
            dma((6,)),
        ],
        name="wing_end",
    )(det, flux, packed)
    return det, flux, face.reshape(1, 1, 4, 5, 16, 32)


def solution(mesh):
    split = Mesh(mesh.devices.reshape(NY, NCORE, NZ, NX), SPAN_CHORD)
    return jax.shard_map(
        on_device,
        mesh=split,
        in_specs=(
            P(None, SPAN_CHORD),
            P(None, SPAN_CHORD),
            P(SPAN_CHORD),
            P(),
            P(),
            P(SPAN_CHORD, None),
            P(None, SPAN_CHORD),
            P(SPAN, CHORD, None, None),
            P(SPAN, CHORD, None, None),
        ),
        out_specs=(
            P(None, None, SPAN_CHORD),
            P(None, None, None, SPAN_CHORD),
            P(SPAN, CHORD, None, None, None, None),
        ),
        check_vma=False,
    )
```
